32 devices in a mesh: rows: 2 (over y), cols: 4 (over z), slabs: 2 (over x), trial: 2 (over core).
Axes of the slice: x: 2, y: 2, z: 4, core: 2. Of those that a mesh axis runs over, the one named last changes fastest.
Arguments:
- field_values: float32 [64, 16, 256, 128], P(('trial', 'rows'), 'cols', 'slabs'), parts along dimension 0, may hold values from 0.5 to 2
- conductance: float32 [64, 16, 256, 128], P(('trial', 'rows'), 'cols', 'slabs'), parts along dimension 0, may hold values from 0.03 to 0.15
- source: float32 [64, 16, 256, 128], P(('trial', 'rows'), 'cols', 'slabs'), parts along dimension 0, may hold values from -0.2 to 0.2
Outputs:
- anomaly: float32 [64, 16, 256, 128], P(('trial', 'rows'), 'cols', 'slabs'), parts along dimension 0
- field_values_end: float32 [64, 16, 256, 128], P(('trial', 'rows'), 'cols', 'slabs'), parts along dimension 0
The draws below stay inside these ranges and needn't reach their ends.
There are 2 independent parts, one for each index of `trial`. The reference program is written for one: setup_inputs(seed, part) draws one part's arguments, and reference() takes and returns one part's arrays. A program takes and returns all parts, laid end to end along the dimension named above; each array names one. Nothing has to cross between parts.
All inputs are finite; a program needn't handle non-finite values.
Results may differ from the reference program's by a relative error of at most 0.00002.
Values sent between devices are 32-bit elements; how exact they have to be, the bound alone decides.
A program may use at most 128 MiB of HBM per device.

```python
import jax
import jax.numpy as jnp
from jax import lax

GRID_J = 32
GRID_I = 16
GRID_K = 256
LEVELS = 128
STEPS = 4


def steps_of(own_key, extent, split, least, largest):
    factor_of, own = 1.0, jax.random.fold_in(own_key, 6)
    for dim, shards_of in split:
        draws = jnp.exp(jax.random.uniform(jax.random.fold_in(own, dim), (shards_of,), jnp.float32, least / len(split), largest / len(split)))
        factor_of = factor_of * jnp.repeat(draws, extent[dim] // shards_of).reshape([-1 if axis == dim else 1 for axis in range(len(extent))])
    return factor_of


def setup_inputs(seed: int = 0, part: int = 0) -> dict:
    keys = jax.random.split(jax.random.key(seed), 4)
    part_splits = jax.random.split(jax.random.fold_in(keys[3], part), 4)
    field_values = jnp.clip(0.5 + 1.5 * jax.random.uniform(part_splits[0], (GRID_J, GRID_I, GRID_K, LEVELS), jnp.float32) ** steps_of(part_splits[0], (GRID_J, GRID_I, GRID_K, LEVELS), ((0, 2), (1, 4), (2, 2)), -0.2, 0.2), 0.5, 2.0)
    conductance = jnp.clip(0.03 + 0.120000007 * jax.random.uniform(part_splits[1], (GRID_J, GRID_I, GRID_K, LEVELS), jnp.float32) ** steps_of(part_splits[1], (GRID_J, GRID_I, GRID_K, LEVELS), ((0, 2), (1, 4), (2, 2)), -0.2, 0.2), 0.03, 0.15)
    source = jnp.clip(jax.random.uniform(part_splits[2], (GRID_J, GRID_I, GRID_K, LEVELS), jnp.float32, -0.2, 0.2) * steps_of(part_splits[2], (GRID_J, GRID_I, GRID_K, LEVELS), ((0, 2), (1, 4), (2, 2)), -0.4, 0.0), -0.2, 0.2)
    return dict(field_values=field_values, conductance=conductance, source=source)


def strip_edges(values, dims):
    for dim in dims:
        values = lax.slice_in_dim(values, 1, values.shape[dim] - 1, axis=dim)
    return values

def neighbour(values, dim, start, dims):
    others = [other for other in dims if other != dim]
    values = strip_edges(values, others)
    return lax.slice_in_dim(values, start, start + values.shape[dim] - 2, axis=dim)

def one_step(padded, conductance, source):
    middle = strip_edges(padded, (0, 1, 2))
    lower = [neighbour(padded, dim, 0, (0, 1, 2)) for dim in (0, 1, 2)]
    upper = [neighbour(padded, dim, 2, (0, 1, 2)) for dim in (0, 1, 2)]
    spread = lower[0] + upper[0] + lower[1] + upper[1] + lower[2] + upper[2] - 6.0 * middle
    return middle + conductance * spread + source

def reference(field_values, conductance, source):
    for step in range(STEPS):
        field_values = one_step(jnp.pad(field_values, ((1, 1), (1, 1), (1, 1), (0, 0)), mode='constant'), conductance, source)
    line_mean = lax.optimization_barrier(jnp.mean(field_values, axis=0, keepdims=True))
    centred = field_values - line_mean
    line_variance = lax.optimization_barrier(jnp.mean(centred * centred, axis=0, keepdims=True))
    anomaly = centred * lax.rsqrt(line_variance + 0.0001)
    return (anomaly, field_values)
```

```python
import functools

import jax
import jax.numpy as jnp
from jax import lax
from jax.experimental import pallas as pl
from jax.experimental.pallas import tpu as pltpu
from jax.sharding import PartitionSpec as P

STEPS = 4
TILE = 8
PIECES = 4
FINE = (5, 2)
SHORT = 128
MESH = pl.DeviceIdType.MESH


def kernel(
    sizes, coarse, parts, field, conductance, source, scaled, last,
    u, cond, src, own, others,
    load_sem, send_sem, recv_sem, jsend_sem, jrecv_sem, ksend_sem, krecv_sem, ssend_sem, srecv_sem,
):
    rows, cols, slabs = sizes
    nj, ni, nk, _ = field.shape
    row, col, slab = (lax.axis_index(name) for name in ("rows", "cols", "slabs"))
    has = {
        "i-": col > 0, "i+": col < cols - 1,
        "j-": row > 0, "j+": row < rows - 1,
        "k-": slab > 0, "k+": slab < slabs - 1,
    }
    to = {
        "i-": {"cols": jnp.maximum(col - 1, 0)}, "i+": {"cols": jnp.minimum(col + 1, cols - 1)},
        "j-": {"rows": jnp.maximum(row - 1, 0)}, "j+": {"rows": jnp.minimum(row + 1, rows - 1)},
        "k-": {"slabs": jnp.maximum(slab - 1, 0)}, "k+": {"slabs": jnp.minimum(slab + 1, slabs - 1)},
    }
    opposite = {"i-": "i+", "i+": "i-", "j-": "j+", "j+": "j-", "k-": "k+", "k+": "k-"}
    descending = lax.rem(slab, 2) == 0

    loads = [
        pltpu.make_async_copy(field, u.at[0, pl.ds(1, nj), pl.ds(1, ni), pl.ds(TILE, nk)], load_sem.at[0]),
        pltpu.make_async_copy(conductance, cond, load_sem.at[1]),
        pltpu.make_async_copy(source, src, load_sem.at[2]),
    ]
    loads[0].start()

    barrier = pltpu.get_barrier_semaphore()
    expected = rows - 1
    for off in range(1, rows):
        pl.semaphore_signal(barrier, inc=1, device_id={"rows": lax.rem(row + off, rows)}, device_id_type=MESH)
    for side in ("i-", "i+", "k-", "k+"):
        expected = expected + jnp.where(has[side], 1, 0)

        @pl.when(has[side])
        def _():
            pl.semaphore_signal(barrier, inc=1, device_id=to[side], device_id_type=MESH)

    pl.semaphore_wait(barrier, expected)

    def start_of(of, n):
        before, size = sum(of[:n]), of[n]
        return pl.multiple_of(jnp.where(descending, nk - before - size, before), TILE)

    def edges_of(n):
        first, final = n == 0, n == len(coarse) - 1
        low = jnp.where(descending, final, first)
        high = jnp.where(descending, first, final)
        return low, high

    def face(side, t, n, first):
        of = parts[t] if side[0] == "i" else coarse
        k0, kq = start_of(of, n), of[n]
        inner = pl.ds(pl.multiple_of(TILE + k0, TILE), kq)
        js, is_ = pl.ds(1, nj), pl.ds(1, ni)
        if side[0] == "i":
            here, there = (1, ni + 1) if side == "i-" else (ni, 0)
            dst = u.at[t, js, there, inner]
            start = field.at[:, here - 1, pl.ds(k0, kq)] if first else u.at[t, js, here, inner]
        else:
            here, there = (1, nj + 1) if side == "j-" else (nj, 0)
            dst = u.at[t, there, is_, inner]
            start = field.at[here - 1, :, pl.ds(k0, kq)] if first else u.at[t, here, is_, inner]
        d = 0 if side[1] == "-" else 1
        sent, received = (send_sem, recv_sem) if side[0] == "i" else (jsend_sem, jrecv_sem)
        return pltpu.make_async_remote_copy(
            src_ref=start, dst_ref=dst, send_sem=sent.at[d, t, n], recv_sem=received.at[d, t, n],
            device_id=to[side], device_id_type=MESH,
        )

    def kface(side, t, first):
        js, is_ = pl.ds(1, nj), pl.ds(1, ni)
        here, there = (TILE, TILE + nk) if side == "k-" else (nk, 0)
        start = field.at[:, :, pl.ds(here - TILE, TILE)] if first else u.at[t, js, is_, pl.ds(here, TILE)]
        d = 0 if side == "k-" else 1
        return pltpu.make_async_remote_copy(
            src_ref=start, dst_ref=u.at[t, js, is_, pl.ds(there, TILE)],
            send_sem=ksend_sem.at[d, t], recv_sem=krecv_sem.at[d, t],
            device_id=to[side], device_id_type=MESH,
        )

    def fine_of(t, n):
        low, done = sum(coarse[:n]), sum(coarse[:n + 1])
        return [m for m in range(len(parts[t])) if low <= sum(parts[t][:m]) < done]

    def send_faces(t, n, first):
        for side in ("i-", "i+"):
            @pl.when(has[side])
            def _():
                for m in fine_of(t, n):
                    face(side, t, m, first).start()

        for side in ("j-", "j+"):
            @pl.when(has[side])
            def _():
                face(side, t, n, first).start()

        low, high = edges_of(n)

        @pl.when(low & has["k-"])
        def _():
            kface("k-", t, first).start()

        @pl.when(high & has["k+"])
        def _():
            kface("k+", t, first).start()

    def wait_i(t, n):
        for side in ("i-", "i+"):
            @pl.when(has[opposite[side]])
            def _():
                face(side, t, n, False).wait_recv()

    def wait_others(t, n):
        for side in ("j-", "j+"):
            @pl.when(has[opposite[side]])
            def _():
                face(side, t, n, False).wait_recv()

        low, high = edges_of(n)

        @pl.when(high & has["k+"])
        def _():
            kface("k-", t, False).wait_recv()

        @pl.when(low & has["k-"])
        def _():
            kface("k+", t, False).wait_recv()

    def wait_sent(t):
        for side in ("i-", "i+"):
            @pl.when(has[side])
            def _():
                for n in range(len(parts[t])):
                    face(side, t, n, False).wait_send()

        for side in ("j-", "j+"):
            @pl.when(has[side])
            def _():
                for n in range(len(coarse)):
                    face(side, t, n, False).wait_send()

        for side in ("k-", "k+"):
            @pl.when(has[side])
            def _():
                kface(side, t, False).wait_send()

    for n in range(len(coarse)):
        send_faces(0, n, True)

    loads[1].start()
    loads[2].start()

    def zero_plane(t, j, i):
        u[t, j, i, pl.ds(TILE, nk)] = jnp.zeros((nk, u.shape[-1]), u.dtype)

    @pl.loop(0, STEPS)
    def _(t):
        for side, i in (("i-", 0), ("i+", ni + 1)):
            @pl.when(jnp.logical_not(has[side]))
            def _():
                @pl.loop(0, nj)
                def _(j):
                    zero_plane(t, j + 1, i)

        for side, j in (("j-", 0), ("j+", nj + 1)):
            @pl.when(jnp.logical_not(has[side]))
            def _():
                for i in range(ni):
                    zero_plane(t, j, i + 1)

        for side, k in (("k-", 0), ("k+", TILE + nk)):
            @pl.when(jnp.logical_not(has[side]))
            def _():
                @pl.loop(0, nj)
                def _(j):
                    for i in range(ni):
                        u[t, j + 1, i + 1, pl.ds(k, TILE)] = jnp.zeros((TILE, u.shape[-1]), u.dtype)

    for load in loads:
        load.wait()

    def stencil(t, j, i, k0, kq):
        inner = pl.ds(pl.multiple_of(TILE + k0, TILE), kq)
        tall = u[t, j + 1, i + 1, pl.ds(k0, kq + 2 * TILE)]
        middle = tall[TILE:TILE + kq]
        spread = u[t, j, i + 1, inner] + u[t, j + 2, i + 1, inner]
        spread = spread + u[t, j + 1, i, inner] + u[t, j + 1, i + 2, inner]
        spread = spread + tall[TILE - 1:TILE - 1 + kq] + tall[TILE + 1:TILE + 1 + kq]
        spread = spread - 6.0 * middle
        own_k = pl.ds(k0, kq)
        return middle + cond[j, i, own_k] * spread + src[j, i, own_k]

    def middle_step(t, n):
        k0, kq = start_of(coarse, n), coarse[n]
        for m in fine_of(t, n):
            wait_i(t, m)
        wait_others(t, n)

        @pl.loop(0, nj)
        def _(jj):
            j = lax.rem(jj + nj - 1, nj)
            for i in range(ni):
                u[t + 1, j + 1, i + 1, pl.ds(pl.multiple_of(TILE + k0, TILE), kq)] = stencil(t, j, i, k0, kq)

        send_faces(t + 1, n, False)

    for t in range(STEPS - 1):
        for n in range(len(coarse)):
            middle_step(t, n)
        if t > 0:
            wait_sent(t - 1)

    t = STEPS - 1
    final = parts[t]
    outer = tuple(range(ni)) if ni < 3 else (0, ni - 1)
    inner = tuple(range(1, ni - 1)) if ni > 2 else ()
    groups = [(outer, 0, final, n, n) for n in range(len(final))]
    if inner:
        groups = [(inner, len(outer), coarse, n, len(final) + n) for n in range(len(coarse))] + groups

    def stats_copy(off, group):
        planes, at, of, n, sem = group
        place = (slice(None), pl.ds(at, len(planes)), pl.ds(start_of(of, n), of[n]))
        return pltpu.make_async_remote_copy(
            src_ref=own.at[place], dst_ref=others.at[(off - 1,) + place],
            send_sem=ssend_sem.at[off - 1, sem], recv_sem=srecv_sem.at[off - 1, sem],
            device_id={"rows": lax.rem(row + off, rows)}, device_id_type=MESH,
        )

    def final_step(group):
        planes, at, of, n, _ = group
        k0, kq = start_of(of, n), of[n]
        ks = pl.ds(k0, kq)
        zero = jnp.zeros((kq, u.shape[-1]), u.dtype)
        for p, i in enumerate(planes):
            if kq * nj <= SHORT:
                news = [stencil(t, j, i, k0, kq) for j in range(nj)]
                mean = sum(news[1:], news[0]) / nj
                own[0, at + p, ks] = mean
                aways = [new - mean for new in news]
                squares = [away * away for away in aways]
                own[1, at + p, ks] = sum(squares[1:], squares[0])
                for j in range(nj):
                    last[j, i, ks] = news[j]
                continue

            def step(j, total):
                new = stencil(t, j, i, k0, kq)
                last[j, i, ks] = new
                return total + new

            mean = lax.fori_loop(0, nj, step, zero, unroll=2) / nj
            own[0, at + p, ks] = mean

            def spread_of(j, total):
                away = last[j, i, ks] - mean
                return total + away * away

            own[1, at + p, ks] = lax.fori_loop(0, nj, spread_of, zero, unroll=2)
        for off in range(1, rows):
            stats_copy(off, group).start()

    def finish(group):
        planes, at, of, n, _ = group
        kq = of[n]
        ks = pl.ds(start_of(of, n), kq)
        for off in range(1, rows):
            stats_copy(off, group).wait_recv()
        for p, i in enumerate(planes):
            means = [own[0, at + p, ks]] + [others[off - 1, 0, at + p, ks] for off in range(1, rows)]
            spreads = [own[1, at + p, ks]] + [others[off - 1, 1, at + p, ks] for off in range(1, rows)]
            mean = sum(means[1:], means[0]) / rows
            spread = sum(spreads[1:], spreads[0])
            for other in means:
                spread = spread + nj * ((other - mean) * (other - mean))
            scale = lax.rsqrt(spread / (nj * rows) + 0.0001)
            if kq * nj <= SHORT:
                for j in range(nj):
                    scaled[j, i, ks] = (last[j, i, ks] - mean) * scale
                continue

            @pl.loop(0, nj)
            def _(j):
                scaled[j, i, ks] = (last[j, i, ks] - mean) * scale

    for n in range(len(coarse)):
        wait_others(t, n)
    for at, group in enumerate(groups):
        if group[0] is outer:
            wait_i(t, group[3])
        final_step(group)
        if at > 0:
            finish(groups[at - 1])
        if at == len(groups) - 2:
            wait_sent(STEPS - 2)
    finish(groups[-1])

    wait_sent(t)
    for group in groups:
        for off in range(1, rows):
            stats_copy(off, group).wait_send()


def write_out(near_anomaly, near_field, anomaly, field_end, sems):
    copies = []
    for which, (start, dst) in enumerate(((near_field, field_end), (near_anomaly, anomaly))):
        pieces = sems.shape[1]
        depth = start.shape[0] // pieces
        for piece in range(pieces):
            js = pl.ds(piece * depth, depth)
            copies.append(pltpu.make_async_copy(start.at[js], dst.at[js], sems.at[which, piece]))
    for copy in copies:
        copy.start()
    for copy in copies:
        copy.wait()


def parts_of(nk):
    half = nk // 2 if nk % (2 * TILE) == 0 else nk
    coarse = (half,) * (nk // half)
    fine, left = [], half
    for eighths in FINE:
        size = half * eighths // 8 // TILE * TILE
        if 0 < size < left:
            fine.append(size)
            left -= size
    return coarse, (coarse,) * (STEPS - 1) + (coarse[:-1] + tuple(fine) + (left,),)


def on_device(field_values, conductance, source):
    sizes = tuple(lax.axis_size(name) for name in ("rows", "cols", "slabs"))
    nj, ni, nk, levels = field_values.shape
    coarse, parts = parts_of(nk)
    most = max(len(of) for of in parts)
    groups = len(parts[-1]) + len(coarse)
    peers = max(sizes[0] - 1, 1)
    whole = pltpu.VMEM(field_values.shape, field_values.dtype)
    near = pl.BlockSpec(memory_space=pltpu.VMEM)
    anywhere = pl.BlockSpec(memory_space=pl.ANY)
    results = pl.pallas_call(
        functools.partial(kernel, sizes, coarse, parts),
        out_shape=(whole, whole),
        in_specs=[anywhere] * 3,
        out_specs=(near, near),
        scratch_shapes=[
            pltpu.VMEM((STEPS, nj + 2, ni + 2, nk + 2 * TILE, levels), jnp.float32),
            pltpu.VMEM((nj, ni, nk, levels), jnp.float32),
            pltpu.VMEM((nj, ni, nk, levels), jnp.float32),
            pltpu.VMEM((2, ni, nk, levels), jnp.float32),
            pltpu.VMEM((peers, 2, ni, nk, levels), jnp.float32),
            pltpu.SemaphoreType.DMA((3,)),
            pltpu.SemaphoreType.DMA((2, STEPS, most)),
            pltpu.SemaphoreType.DMA((2, STEPS, most)),
            pltpu.SemaphoreType.DMA((2, STEPS, len(coarse))),
            pltpu.SemaphoreType.DMA((2, STEPS, len(coarse))),
            pltpu.SemaphoreType.DMA((2, STEPS)),
            pltpu.SemaphoreType.DMA((2, STEPS)),
            pltpu.SemaphoreType.DMA((peers, groups)),
            pltpu.SemaphoreType.DMA((peers, groups)),
        ],
        compiler_params=pltpu.CompilerParams(
            collective_id=0, has_side_effects=True, vmem_limit_bytes=52 * 1024 * 1024
        ),
        name="heat_steps",
    )(field_values, conductance, source)
    there = jax.ShapeDtypeStruct(field_values.shape, field_values.dtype)
    pieces = PIECES if nj % PIECES == 0 else 1
    return pl.pallas_call(
        write_out,
        out_shape=(there, there),
        in_specs=[near] * 2,
        out_specs=(anywhere, anywhere),
        scratch_shapes=[pltpu.SemaphoreType.DMA((2, pieces))],
        compiler_params=pltpu.CompilerParams(vmem_limit_bytes=1024 * 1024),
        name="write_out",
    )(*results)


def solution(mesh):
    spec = P(("trial", "rows"), "cols", "slabs", None)
    return jax.shard_map(
        on_device, mesh=mesh, in_specs=(spec,) * 3, out_specs=(spec, spec), check_vma=False
    )
```

```python
import functools

import jax
import jax.numpy as jnp
from jax import lax
from jax.experimental import pallas as pl
from jax.experimental.pallas import tpu as pltpu
from jax.sharding import PartitionSpec as P

STEPS = 4
TILE = 8
PIECES = 4
FINE = (5, 2)
SHORT = 128
YIELD = 1
PAUSE = 2000
MESH = pl.DeviceIdType.MESH


def kernel(
    sizes, coarse, parts, field, conductance, source, scaled, last,
    u, cond, src, own, others,
    load_sem, send_sem, recv_sem, jsend_sem, jrecv_sem, ksend_sem, krecv_sem, ssend_sem, srecv_sem,
):
    rows, cols, slabs = sizes
    nj, ni, nk, _ = field.shape
    row, col, slab = (lax.axis_index(name) for name in ("rows", "cols", "slabs"))
    has = {
        "i-": col > 0, "i+": col < cols - 1,
        "j-": row > 0, "j+": row < rows - 1,
        "k-": slab > 0, "k+": slab < slabs - 1,
    }
    to = {
        "i-": {"cols": jnp.maximum(col - 1, 0)}, "i+": {"cols": jnp.minimum(col + 1, cols - 1)},
        "j-": {"rows": jnp.maximum(row - 1, 0)}, "j+": {"rows": jnp.minimum(row + 1, rows - 1)},
        "k-": {"slabs": jnp.maximum(slab - 1, 0)}, "k+": {"slabs": jnp.minimum(slab + 1, slabs - 1)},
    }
    opposite = {"i-": "i+", "i+": "i-", "j-": "j+", "j+": "j-", "k-": "k+", "k+": "k-"}
    first_core = lax.rem(lax.axis_index("trial"), 2) == 0
    descending = lax.rem(slab, 2) == 0

    loads = [
        pltpu.make_async_copy(field, u.at[0, pl.ds(1, nj), pl.ds(1, ni), pl.ds(TILE, nk)], load_sem.at[0]),
        pltpu.make_async_copy(conductance, cond, load_sem.at[1]),
        pltpu.make_async_copy(source, src, load_sem.at[2]),
    ]
    loads[0].start()

    barrier = pltpu.get_barrier_semaphore()
    expected = rows - 1
    for off in range(1, rows):
        pl.semaphore_signal(barrier, inc=1, device_id={"rows": lax.rem(row + off, rows)}, device_id_type=MESH)
    for side in ("i-", "i+", "k-", "k+"):
        expected = expected + jnp.where(has[side], 1, 0)

        @pl.when(has[side])
        def _():
            pl.semaphore_signal(barrier, inc=1, device_id=to[side], device_id_type=MESH)

    pl.semaphore_wait(barrier, expected)

    def start_of(of, n):
        before, size = sum(of[:n]), of[n]
        return pl.multiple_of(jnp.where(descending, nk - before - size, before), TILE)

    def edges_of(n):
        first, final = n == 0, n == len(coarse) - 1
        low = jnp.where(descending, final, first)
        high = jnp.where(descending, first, final)
        return low, high

    def face(side, t, n, first):
        of = parts[t] if side[0] == "i" else coarse
        k0, kq = start_of(of, n), of[n]
        inner = pl.ds(pl.multiple_of(TILE + k0, TILE), kq)
        js, is_ = pl.ds(1, nj), pl.ds(1, ni)
        if side[0] == "i":
            here, there = (1, ni + 1) if side == "i-" else (ni, 0)
            dst = u.at[t, js, there, inner]
            start = field.at[:, here - 1, pl.ds(k0, kq)] if first else u.at[t, js, here, inner]
        else:
            here, there = (1, nj + 1) if side == "j-" else (nj, 0)
            dst = u.at[t, there, is_, inner]
            start = field.at[here - 1, :, pl.ds(k0, kq)] if first else u.at[t, here, is_, inner]
        d = 0 if side[1] == "-" else 1
        sent, received = (send_sem, recv_sem) if side[0] == "i" else (jsend_sem, jrecv_sem)
        return pltpu.make_async_remote_copy(
            src_ref=start, dst_ref=dst, send_sem=sent.at[d, t, n], recv_sem=received.at[d, t, n],
            device_id=to[side], device_id_type=MESH,
        )

    def kface(side, t, first):
        js, is_ = pl.ds(1, nj), pl.ds(1, ni)
        here, there = (TILE, TILE + nk) if side == "k-" else (nk, 0)
        start = field.at[:, :, pl.ds(here - TILE, TILE)] if first else u.at[t, js, is_, pl.ds(here, TILE)]
        d = 0 if side == "k-" else 1
        return pltpu.make_async_remote_copy(
            src_ref=start, dst_ref=u.at[t, js, is_, pl.ds(there, TILE)],
            send_sem=ksend_sem.at[d, t], recv_sem=krecv_sem.at[d, t],
            device_id=to[side], device_id_type=MESH,
        )

    def fine_of(t, n):
        low, done = sum(coarse[:n]), sum(coarse[:n + 1])
        return [m for m in range(len(parts[t])) if low <= sum(parts[t][:m]) < done]

    def send_faces(t, n, first):
        for side in ("i-", "i+"):
            @pl.when(has[side])
            def _():
                for m in fine_of(t, n):
                    face(side, t, m, first).start()

        for side in ("j-", "j+"):
            @pl.when(has[side])
            def _():
                face(side, t, n, first).start()

        low, high = edges_of(n)

        @pl.when(low & has["k-"])
        def _():
            kface("k-", t, first).start()

        @pl.when(high & has["k+"])
        def _():
            kface("k+", t, first).start()

    def wait_i(t, n):
        for side in ("i-", "i+"):
            @pl.when(has[opposite[side]])
            def _():
                face(side, t, n, False).wait_recv()

    def wait_others(t, n):
        for side in ("j-", "j+"):
            @pl.when(has[opposite[side]])
            def _():
                face(side, t, n, False).wait_recv()

        low, high = edges_of(n)

        @pl.when(high & has["k+"])
        def _():
            kface("k-", t, False).wait_recv()

        @pl.when(low & has["k-"])
        def _():
            kface("k+", t, False).wait_recv()

    def wait_sent_i(t, who):
        for side in ("i-", "i+"):
            @pl.when(who & has[side])
            def _():
                for n in range(len(parts[t])):
                    face(side, t, n, False).wait_send()

    def wait_sent(t):
        wait_sent_i(t, first_core if t == YIELD else True)
        for side in ("j-", "j+"):
            @pl.when(has[side])
            def _():
                for n in range(len(coarse)):
                    face(side, t, n, False).wait_send()

        for side in ("k-", "k+"):
            @pl.when(has[side])
            def _():
                kface(side, t, False).wait_send()

    for n in range(len(coarse)):
        send_faces(0, n, True)

    loads[1].start()
    loads[2].start()

    def zero_plane(t, j, i):
        u[t, j, i, pl.ds(TILE, nk)] = jnp.zeros((nk, u.shape[-1]), u.dtype)

    @pl.loop(0, STEPS)
    def _(t):
        for side, i in (("i-", 0), ("i+", ni + 1)):
            @pl.when(jnp.logical_not(has[side]))
            def _():
                @pl.loop(0, nj)
                def _(j):
                    zero_plane(t, j + 1, i)

        for side, j in (("j-", 0), ("j+", nj + 1)):
            @pl.when(jnp.logical_not(has[side]))
            def _():
                for i in range(ni):
                    zero_plane(t, j, i + 1)

        for side, k in (("k-", 0), ("k+", TILE + nk)):
            @pl.when(jnp.logical_not(has[side]))
            def _():
                @pl.loop(0, nj)
                def _(j):
                    for i in range(ni):
                        u[t, j + 1, i + 1, pl.ds(k, TILE)] = jnp.zeros((TILE, u.shape[-1]), u.dtype)

    for load in loads:
        load.wait()

    def stencil(t, j, i, k0, kq):
        inner = pl.ds(pl.multiple_of(TILE + k0, TILE), kq)
        tall = u[t, j + 1, i + 1, pl.ds(k0, kq + 2 * TILE)]
        middle = tall[TILE:TILE + kq]
        spread = u[t, j, i + 1, inner] + u[t, j + 2, i + 1, inner]
        spread = spread + u[t, j + 1, i, inner] + u[t, j + 1, i + 2, inner]
        spread = spread + tall[TILE - 1:TILE - 1 + kq] + tall[TILE + 1:TILE + 1 + kq]
        spread = spread - 6.0 * middle
        own_k = pl.ds(k0, kq)
        return middle + cond[j, i, own_k] * spread + src[j, i, own_k]

    def middle_step(t, n):
        k0, kq = start_of(coarse, n), coarse[n]
        for m in fine_of(t, n):
            wait_i(t, m)
        wait_others(t, n)

        @pl.loop(0, nj)
        def _(jj):
            j = lax.rem(jj + nj - 1, nj)
            for i in range(ni):
                u[t + 1, j + 1, i + 1, pl.ds(pl.multiple_of(TILE + k0, TILE), kq)] = stencil(t, j, i, k0, kq)

        if t == YIELD and n == 0:
            wait_sent_i(t, jnp.logical_not(first_core))

            @pl.when(jnp.logical_not(first_core))
            def _():
                pl.delay(PAUSE)

        send_faces(t + 1, n, False)

    for t in range(STEPS - 1):
        for n in range(len(coarse)):
            middle_step(t, n)
        if t > 0:
            wait_sent(t - 1)

    t = STEPS - 1
    final = parts[t]
    outer = tuple(range(ni)) if ni < 3 else (0, ni - 1)
    inner = tuple(range(1, ni - 1)) if ni > 2 else ()
    groups = [(outer, 0, final, n, n) for n in range(len(final))]
    if inner:
        groups = [(inner, len(outer), coarse, n, len(final) + n) for n in range(len(coarse))] + groups

    def stats_copy(off, group):
        planes, at, of, n, sem = group
        place = (slice(None), pl.ds(at, len(planes)), pl.ds(start_of(of, n), of[n]))
        return pltpu.make_async_remote_copy(
            src_ref=own.at[place], dst_ref=others.at[(off - 1,) + place],
            send_sem=ssend_sem.at[off - 1, sem], recv_sem=srecv_sem.at[off - 1, sem],
            device_id={"rows": lax.rem(row + off, rows)}, device_id_type=MESH,
        )

    def final_step(group):
        planes, at, of, n, _ = group
        k0, kq = start_of(of, n), of[n]
        ks = pl.ds(k0, kq)
        zero = jnp.zeros((kq, u.shape[-1]), u.dtype)
        for p, i in enumerate(planes):
            if kq * nj <= SHORT:
                news = [stencil(t, j, i, k0, kq) for j in range(nj)]
                mean = sum(news[1:], news[0]) / nj
                own[0, at + p, ks] = mean
                aways = [new - mean for new in news]
                squares = [away * away for away in aways]
                own[1, at + p, ks] = sum(squares[1:], squares[0])
                for j in range(nj):
                    last[j, i, ks] = news[j]
                continue

            def step(j, total):
                new = stencil(t, j, i, k0, kq)
                last[j, i, ks] = new
                return total + new

            mean = lax.fori_loop(0, nj, step, zero, unroll=2) / nj
            own[0, at + p, ks] = mean

            def spread_of(j, total):
                away = last[j, i, ks] - mean
                return total + away * away

            own[1, at + p, ks] = lax.fori_loop(0, nj, spread_of, zero, unroll=2)
        for off in range(1, rows):
            stats_copy(off, group).start()

    def finish(group):
        planes, at, of, n, _ = group
        kq = of[n]
        ks = pl.ds(start_of(of, n), kq)
        for off in range(1, rows):
            stats_copy(off, group).wait_recv()
        for p, i in enumerate(planes):
            means = [own[0, at + p, ks]] + [others[off - 1, 0, at + p, ks] for off in range(1, rows)]
            spreads = [own[1, at + p, ks]] + [others[off - 1, 1, at + p, ks] for off in range(1, rows)]
            mean = sum(means[1:], means[0]) / rows
            spread = sum(spreads[1:], spreads[0])
            for other in means:
                spread = spread + nj * ((other - mean) * (other - mean))
            scale = lax.rsqrt(spread / (nj * rows) + 0.0001)
            if kq * nj <= SHORT:
                for j in range(nj):
                    scaled[j, i, ks] = (last[j, i, ks] - mean) * scale
                continue

            @pl.loop(0, nj)
            def _(j):
                scaled[j, i, ks] = (last[j, i, ks] - mean) * scale

    for n in range(len(coarse)):
        wait_others(t, n)
    for at, group in enumerate(groups):
        if group[0] is outer:
            wait_i(t, group[3])
        final_step(group)
        if at > 0:
            finish(groups[at - 1])
        if at == len(groups) - 2:
            wait_sent(STEPS - 2)
    finish(groups[-1])

    wait_sent(t)
    for group in groups:
        for off in range(1, rows):
            stats_copy(off, group).wait_send()


def write_out(near_anomaly, near_field, anomaly, field_end, sems):
    copies = []
    for which, (start, dst) in enumerate(((near_field, field_end), (near_anomaly, anomaly))):
        pieces = sems.shape[1]
        depth = start.shape[0] // pieces
        for piece in range(pieces):
            js = pl.ds(piece * depth, depth)
            copies.append(pltpu.make_async_copy(start.at[js], dst.at[js], sems.at[which, piece]))
    for copy in copies:
        copy.start()
    for copy in copies:
        copy.wait()


def parts_of(nk):
    half = nk // 2 if nk % (2 * TILE) == 0 else nk
    coarse = (half,) * (nk // half)
    fine, left = [], half
    for eighths in FINE:
        size = half * eighths // 8 // TILE * TILE
        if 0 < size < left:
            fine.append(size)
            left -= size
    return coarse, (coarse,) * (STEPS - 1) + (coarse[:-1] + tuple(fine) + (left,),)


def on_device(field_values, conductance, source):
    sizes = tuple(lax.axis_size(name) for name in ("rows", "cols", "slabs"))
    nj, ni, nk, levels = field_values.shape
    coarse, parts = parts_of(nk)
    most = max(len(of) for of in parts)
    groups = len(parts[-1]) + len(coarse)
    peers = max(sizes[0] - 1, 1)
    whole = pltpu.VMEM(field_values.shape, field_values.dtype)
    near = pl.BlockSpec(memory_space=pltpu.VMEM)
    anywhere = pl.BlockSpec(memory_space=pl.ANY)
    results = pl.pallas_call(
        functools.partial(kernel, sizes, coarse, parts),
        out_shape=(whole, whole),
        in_specs=[anywhere] * 3,
        out_specs=(near, near),
        scratch_shapes=[
            pltpu.VMEM((STEPS, nj + 2, ni + 2, nk + 2 * TILE, levels), jnp.float32),
            pltpu.VMEM((nj, ni, nk, levels), jnp.float32),
            pltpu.VMEM((nj, ni, nk, levels), jnp.float32),
            pltpu.VMEM((2, ni, nk, levels), jnp.float32),
            pltpu.VMEM((peers, 2, ni, nk, levels), jnp.float32),
            pltpu.SemaphoreType.DMA((3,)),
            pltpu.SemaphoreType.DMA((2, STEPS, most)),
            pltpu.SemaphoreType.DMA((2, STEPS, most)),
            pltpu.SemaphoreType.DMA((2, STEPS, len(coarse))),
            pltpu.SemaphoreType.DMA((2, STEPS, len(coarse))),
            pltpu.SemaphoreType.DMA((2, STEPS)),
            pltpu.SemaphoreType.DMA((2, STEPS)),
            pltpu.SemaphoreType.DMA((peers, groups)),
            pltpu.SemaphoreType.DMA((peers, groups)),
        ],
        compiler_params=pltpu.CompilerParams(
            collective_id=0, has_side_effects=True, vmem_limit_bytes=52 * 1024 * 1024
        ),
        name="heat_steps",
    )(field_values, conductance, source)
    there = jax.ShapeDtypeStruct(field_values.shape, field_values.dtype)
    pieces = PIECES if nj % PIECES == 0 else 1
    return pl.pallas_call(
        write_out,
        out_shape=(there, there),
        in_specs=[near] * 2,
        out_specs=(anywhere, anywhere),
        scratch_shapes=[pltpu.SemaphoreType.DMA((2, pieces))],
        compiler_params=pltpu.CompilerParams(vmem_limit_bytes=1024 * 1024),
        name="write_out",
    )(*results)


def solution(mesh):
    spec = P(("trial", "rows"), "cols", "slabs", None)
    return jax.shard_map(
        on_device, mesh=mesh, in_specs=(spec,) * 3, out_specs=(spec, spec), check_vma=False
    )
```

```python
import functools

import jax
import jax.numpy as jnp
from jax import lax
from jax.experimental import pallas as pl
from jax.experimental.pallas import tpu as pltpu
from jax.sharding import PartitionSpec as P

STEPS = 4
TILE = 8
PIECES = 4
FINE = (4,)
YIELD = 1
PAUSE = 2000
MESH = pl.DeviceIdType.MESH


def kernel(
    sizes, coarse, parts, field, conductance, source, scaled, last, late,
    u, cond, src, own, others,
    load_sem, send_sem, recv_sem, jsend_sem, jrecv_sem, ksend_sem, krecv_sem, ssend_sem, srecv_sem,
):
    rows, cols, slabs = sizes
    nj, ni, nk, _ = field.shape
    row, col, slab = (lax.axis_index(name) for name in ("rows", "cols", "slabs"))
    has = {
        "i-": col > 0, "i+": col < cols - 1,
        "j-": row > 0, "j+": row < rows - 1,
        "k-": slab > 0, "k+": slab < slabs - 1,
    }
    to = {
        "i-": {"cols": jnp.maximum(col - 1, 0)}, "i+": {"cols": jnp.minimum(col + 1, cols - 1)},
        "j-": {"rows": jnp.maximum(row - 1, 0)}, "j+": {"rows": jnp.minimum(row + 1, rows - 1)},
        "k-": {"slabs": jnp.maximum(slab - 1, 0)}, "k+": {"slabs": jnp.minimum(slab + 1, slabs - 1)},
    }
    opposite = {"i-": "i+", "i+": "i-", "j-": "j+", "j+": "j-", "k-": "k+", "k+": "k-"}
    first_core = lax.rem(lax.axis_index("trial"), 2) == 0
    descending = lax.rem(slab, 2) == 0

    loads = [
        pltpu.make_async_copy(field, u.at[0, pl.ds(1, nj), pl.ds(1, ni), pl.ds(TILE, nk)], load_sem.at[0]),
        pltpu.make_async_copy(conductance, cond, load_sem.at[1]),
        pltpu.make_async_copy(source, src, load_sem.at[2]),
    ]
    loads[0].start()

    barrier = pltpu.get_barrier_semaphore()
    expected = rows - 1
    for off in range(1, rows):
        pl.semaphore_signal(barrier, inc=1, device_id={"rows": lax.rem(row + off, rows)}, device_id_type=MESH)
    for side in ("i-", "i+", "k-", "k+"):
        expected = expected + jnp.where(has[side], 1, 0)

        @pl.when(has[side])
        def _():
            pl.semaphore_signal(barrier, inc=1, device_id=to[side], device_id_type=MESH)

    pl.semaphore_wait(barrier, expected)

    def start_of(of, n):
        before, size = sum(of[:n]), of[n]
        return pl.multiple_of(jnp.where(descending, nk - before - size, before), TILE)

    def edges_of(n):
        first, final = n == 0, n == len(coarse) - 1
        low = jnp.where(descending, final, first)
        high = jnp.where(descending, first, final)
        return low, high

    def face(side, t, n, first):
        of = parts[t] if side[0] == "i" else coarse
        k0, kq = start_of(of, n), of[n]
        inner = pl.ds(pl.multiple_of(TILE + k0, TILE), kq)
        js, is_ = pl.ds(1, nj), pl.ds(1, ni)
        if side[0] == "i":
            here, there = (1, ni + 1) if side == "i-" else (ni, 0)
            dst = u.at[t, js, there, inner]
            start = field.at[:, here - 1, pl.ds(k0, kq)] if first else u.at[t, js, here, inner]
        else:
            here, there = (1, nj + 1) if side == "j-" else (nj, 0)
            dst = u.at[t, there, is_, inner]
            start = field.at[here - 1, :, pl.ds(k0, kq)] if first else u.at[t, here, is_, inner]
        d = 0 if side[1] == "-" else 1
        sent, received = (send_sem, recv_sem) if side[0] == "i" else (jsend_sem, jrecv_sem)
        return pltpu.make_async_remote_copy(
            src_ref=start, dst_ref=dst, send_sem=sent.at[d, t, n], recv_sem=received.at[d, t, n],
            device_id=to[side], device_id_type=MESH,
        )

    def kface(side, t, first):
        js, is_ = pl.ds(1, nj), pl.ds(1, ni)
        here, there = (TILE, TILE + nk) if side == "k-" else (nk, 0)
        start = field.at[:, :, pl.ds(here - TILE, TILE)] if first else u.at[t, js, is_, pl.ds(here, TILE)]
        d = 0 if side == "k-" else 1
        return pltpu.make_async_remote_copy(
            src_ref=start, dst_ref=u.at[t, js, is_, pl.ds(there, TILE)],
            send_sem=ksend_sem.at[d, t], recv_sem=krecv_sem.at[d, t],
            device_id=to[side], device_id_type=MESH,
        )

    def fine_of(t, n):
        low, done = sum(coarse[:n]), sum(coarse[:n + 1])
        return [m for m in range(len(parts[t])) if low <= sum(parts[t][:m]) < done]

    def send_faces(t, n, first):
        for side in ("i-", "i+"):
            @pl.when(has[side])
            def _():
                for m in fine_of(t, n):
                    face(side, t, m, first).start()

        for side in ("j-", "j+"):
            @pl.when(has[side])
            def _():
                face(side, t, n, first).start()

        low, high = edges_of(n)

        @pl.when(low & has["k-"])
        def _():
            kface("k-", t, first).start()

        @pl.when(high & has["k+"])
        def _():
            kface("k+", t, first).start()

    def wait_i(t, n):
        for side in ("i-", "i+"):
            @pl.when(has[opposite[side]])
            def _():
                face(side, t, n, False).wait_recv()

    def wait_others(t, n):
        for side in ("j-", "j+"):
            @pl.when(has[opposite[side]])
            def _():
                face(side, t, n, False).wait_recv()

        low, high = edges_of(n)

        @pl.when(high & has["k+"])
        def _():
            kface("k-", t, False).wait_recv()

        @pl.when(low & has["k-"])
        def _():
            kface("k+", t, False).wait_recv()

    def wait_sent_i(t, who):
        for side in ("i-", "i+"):
            @pl.when(who & has[side])
            def _():
                for n in range(len(parts[t])):
                    face(side, t, n, False).wait_send()

    def wait_sent(t):
        wait_sent_i(t, first_core if t == YIELD else True)
        for side in ("j-", "j+"):
            @pl.when(has[side])
            def _():
                for n in range(len(coarse)):
                    face(side, t, n, False).wait_send()

        for side in ("k-", "k+"):
            @pl.when(has[side])
            def _():
                kface(side, t, False).wait_send()

    for n in range(len(coarse)):
        send_faces(0, n, True)

    loads[1].start()
    loads[2].start()

    def zero_plane(t, j, i):
        u[t, j, i, pl.ds(TILE, nk)] = jnp.zeros((nk, u.shape[-1]), u.dtype)

    @pl.loop(0, STEPS)
    def _(t):
        for side, i in (("i-", 0), ("i+", ni + 1)):
            @pl.when(jnp.logical_not(has[side]))
            def _():
                @pl.loop(0, nj)
                def _(j):
                    zero_plane(t, j + 1, i)

        for side, j in (("j-", 0), ("j+", nj + 1)):
            @pl.when(jnp.logical_not(has[side]))
            def _():
                for i in range(ni):
                    zero_plane(t, j, i + 1)

        for side, k in (("k-", 0), ("k+", TILE + nk)):
            @pl.when(jnp.logical_not(has[side]))
            def _():
                @pl.loop(0, nj)
                def _(j):
                    for i in range(ni):
                        u[t, j + 1, i + 1, pl.ds(k, TILE)] = jnp.zeros((TILE, u.shape[-1]), u.dtype)

    for load in loads:
        load.wait()

    def stencil(t, j, i, k0, kq, skip=(False, False)):
        inner = pl.ds(pl.multiple_of(TILE + k0, TILE), kq)
        tall = u[t, j + 1, i + 1, pl.ds(k0, kq + 2 * TILE)]
        middle = tall[TILE:TILE + kq]
        spread = u[t, j, i + 1, inner] + u[t, j + 2, i + 1, inner]
        for beside, left_out in ((i, skip[0]), (i + 2, skip[1])):
            if not left_out:
                spread = spread + u[t, j + 1, beside, inner]
        spread = spread + tall[TILE - 1:TILE - 1 + kq] + tall[TILE + 1:TILE + 1 + kq]
        spread = spread - 6.0 * middle
        own_k = pl.ds(k0, kq)
        return middle + cond[j, i, own_k] * spread + src[j, i, own_k]

    def middle_step(t, n):
        k0, kq = start_of(coarse, n), coarse[n]
        for m in fine_of(t, n):
            wait_i(t, m)
        wait_others(t, n)

        @pl.loop(0, nj)
        def _(jj):
            j = lax.rem(jj + nj - 1, nj)
            for i in range(ni):
                u[t + 1, j + 1, i + 1, pl.ds(pl.multiple_of(TILE + k0, TILE), kq)] = stencil(t, j, i, k0, kq)

        if t == YIELD and n == 0:
            wait_sent_i(t, jnp.logical_not(first_core))

            @pl.when(jnp.logical_not(first_core))
            def _():
                pl.delay(PAUSE)

        send_faces(t + 1, n, False)

    for t in range(STEPS - 1):
        for n in range(len(coarse)):
            middle_step(t, n)
        if t > 0:
            wait_sent(t - 1)

    t = STEPS - 1
    final = parts[t]
    outer, inner = planes_of(ni)
    groups = [(inner, len(outer), coarse, n, n) for n in range(len(coarse))] if inner else []
    groups += [(outer, 0, final, n, len(coarse) + n) for n in range(len(final) - 1)]

    def stats_copy(off, group):
        planes, at, of, n, sem = group
        place = (slice(None), pl.ds(at, len(planes)), pl.ds(start_of(of, n), of[n]))
        return pltpu.make_async_remote_copy(
            src_ref=own.at[place], dst_ref=others.at[(off - 1,) + place],
            send_sem=ssend_sem.at[off - 1, sem], recv_sem=srecv_sem.at[off - 1, sem],
            device_id={"rows": lax.rem(row + off, rows)}, device_id_type=MESH,
        )

    def blocks(of, n):
        def wrap(body):
            k0 = start_of(of, n)

            @pl.loop(0, of[n] // TILE)
            def _(b):
                body(pl.multiple_of(k0 + b * TILE, TILE), pl.multiple_of(b * TILE, TILE))
        return wrap

    def sums_of(news):
        mean = sum(news[1:], news[0]) / nj
        aways = [new - mean for new in news]
        squares = [away * away for away in aways]
        return mean, sum(squares[1:], squares[0])

    def inner_step(group):
        planes, at, of, n, _ = group

        @blocks(of, n)
        def _(k, b):
            ks = pl.ds(k, TILE)
            for p, i in enumerate(planes):
                news = [stencil(t, j, i, k, TILE) for j in range(nj)]
                own[0, at + p, ks], own[1, at + p, ks] = sums_of(news)
                for j in range(nj):
                    last[j, i, ks] = news[j]

        for off in range(1, rows):
            stats_copy(off, group).start()

    def outer_ahead(n):
        @blocks(coarse, n)
        def _(k, b):
            for i in outer:
                for j in range(nj):
                    last[j, i, pl.ds(k, TILE)] = stencil(t, j, i, k, TILE, skip=(i == 0, i == ni - 1))

    def outer_step(n, into):
        @blocks(final, n)
        def _(k, b):
            ks, inside = pl.ds(k, TILE), pl.ds(pl.multiple_of(TILE + k, TILE), TILE)
            for p, i in enumerate(outer):
                faces = [face for face, here in ((0, i == 0), (ni + 1, i == ni - 1)) if here]
                news = []
                for j in range(nj):
                    arrived = [u[t, j + 1, face, inside] for face in faces]
                    news.append(last[j, i, ks] + cond[j, i, ks] * sum(arrived[1:], arrived[0]))
                if into is own:
                    own[0, p, ks], own[1, p, ks] = sums_of(news)
                else:
                    into[0, p, pl.ds(b, TILE)], into[1, p, pl.ds(b, TILE)] = sums_of(news)
                for j in range(nj):
                    last[j, i, ks] = news[j]

    def finish(group):
        planes, at, of, n, _ = group
        for off in range(1, rows):
            stats_copy(off, group).wait_recv()

        @blocks(of, n)
        def _(k, b):
            ks = pl.ds(k, TILE)
            for p, i in enumerate(planes):
                means = [own[0, at + p, ks]] + [others[off - 1, 0, at + p, ks] for off in range(1, rows)]
                spreads = [own[1, at + p, ks]] + [others[off - 1, 1, at + p, ks] for off in range(1, rows)]
                mean, scale = joined(nj, means, spreads)
                for j in range(nj):
                    scaled[j, i, ks] = (last[j, i, ks] - mean) * scale

    for n in range(len(coarse)):
        wait_others(t, n)
    count = len(coarse) if inner else 0
    for group in groups[:count]:
        inner_step(group)
    for n in range(len(coarse)):
        outer_ahead(n)
    for group in groups[:count]:
        finish(group)
    wait_sent(STEPS - 2)
    for n in range(len(final) - 1):
        wait_i(t, n)
        outer_step(n, own)
        for off in range(1, rows):
            stats_copy(off, groups[count + n]).start()
        if n > 0:
            finish(groups[count + n - 1])
    wait_i(t, len(final) - 1)
    outer_step(len(final) - 1, late)
    if len(final) > 1:
        finish(groups[-1])
    for group in groups:
        for off in range(1, rows):
            stats_copy(off, group).wait_send()
    wait_sent(t)


def planes_of(ni):
    outer = tuple(range(ni)) if ni < 3 else (0, ni - 1)
    return outer, tuple(i for i in range(ni) if i not in outer)


def joined(nj, means, spreads):
    count = len(means)
    mean = sum(means[1:], means[0]) / count
    spread = sum(spreads[1:], spreads[0])
    for other in means:
        spread = spread + nj * ((other - mean) * (other - mean))
    return mean, lax.rsqrt(spread / (nj * count) + 0.0001)


def write_out(near_anomaly, near_field, anomaly, field_end, sems):
    copies = []
    for which, (start, dst) in enumerate(((near_field, field_end), (near_anomaly, anomaly))):
        pieces = sems.shape[1]
        depth = start.shape[0] // pieces
        for piece in range(pieces):
            js = pl.ds(piece * depth, depth)
            copies.append(pltpu.make_async_copy(start.at[js], dst.at[js], sems.at[which, piece]))
    for copy in copies:
        copy.start()
    for copy in copies:
        copy.wait()


def write_late(before, near_field, late, *refs):
    others, (anomaly, scaled, sems) = refs[:-3], refs[-3:]
    nj, ni, nk, _ = near_field.shape
    size = late.shape[2]
    descending = lax.rem(lax.axis_index("slabs"), 2) == 0
    start = pl.multiple_of(jnp.where(descending, 0, nk - size), TILE)
    copies = []
    for p, i in enumerate(planes_of(ni)[0]):
        @pl.loop(0, size // TILE)
        def _(b):
            ks = pl.ds(pl.multiple_of(b * TILE, TILE), TILE)
            ms = pl.ds(pl.multiple_of(start + b * TILE, TILE), TILE)
            stats = (late,) + others
            mean, scale = joined(nj, [of[0, p, ks] for of in stats], [of[1, p, ks] for of in stats])
            for j in range(nj):
                scaled[p, j, ks] = (near_field[j, i, ms] - mean) * scale

        copies.append(pltpu.make_async_copy(scaled.at[p], anomaly.at[:, i, pl.ds(start, size)], sems.at[p]))
        copies[-1].start()
    for copy in copies:
        copy.wait()


def parts_of(nk):
    half = nk // 2 if nk % (2 * TILE) == 0 else nk
    coarse = (half,) * (nk // half)
    fine, left = [], half
    for eighths in FINE:
        size = half * eighths // 8 // TILE * TILE
        if 0 < size < left:
            fine.append(size)
            left -= size
    return coarse, (coarse,) * (STEPS - 1) + (coarse[:-1] + tuple(fine) + (left,),)


def on_device(field_values, conductance, source):
    sizes = tuple(lax.axis_size(name) for name in ("rows", "cols", "slabs"))
    nj, ni, nk, levels = field_values.shape
    coarse, parts = parts_of(nk)
    most = max(len(of) for of in parts)
    groups = len(parts[-1]) + len(coarse)
    peers = max(sizes[0] - 1, 1)
    whole = pltpu.VMEM(field_values.shape, field_values.dtype)
    near = pl.BlockSpec(memory_space=pltpu.VMEM)
    outer = len(planes_of(ni)[0])
    small = (2, outer, parts[-1][-1], levels)
    anywhere = pl.BlockSpec(memory_space=pl.ANY)
    scaled, last, late = pl.pallas_call(
        functools.partial(kernel, sizes, coarse, parts),
        out_shape=(whole, whole, pltpu.VMEM(small, jnp.float32)),
        in_specs=[anywhere] * 3,
        out_specs=(near, near, near),
        scratch_shapes=[
            pltpu.VMEM((STEPS, nj + 2, ni + 2, nk + 2 * TILE, levels), jnp.float32),
            pltpu.VMEM((nj, ni, nk, levels), jnp.float32),
            pltpu.VMEM((nj, ni, nk, levels), jnp.float32),
            pltpu.VMEM((2, ni, nk, levels), jnp.float32),
            pltpu.VMEM((peers, 2, ni, nk, levels), jnp.float32),
            pltpu.SemaphoreType.DMA((3,)),
            pltpu.SemaphoreType.DMA((2, STEPS, most)),
            pltpu.SemaphoreType.DMA((2, STEPS, most)),
            pltpu.SemaphoreType.DMA((2, STEPS, len(coarse))),
            pltpu.SemaphoreType.DMA((2, STEPS, len(coarse))),
            pltpu.SemaphoreType.DMA((2, STEPS)),
            pltpu.SemaphoreType.DMA((2, STEPS)),
            pltpu.SemaphoreType.DMA((peers, groups)),
            pltpu.SemaphoreType.DMA((peers, groups)),
        ],
        compiler_params=pltpu.CompilerParams(
            collective_id=0, has_side_effects=True, vmem_limit_bytes=52 * 1024 * 1024
        ),
        name="heat_steps",
    )(field_values, conductance, source)
    n = sizes[0]
    others = [lax.ppermute(late, "rows", [(r, (r + off) % n) for r in range(n)]) for off in range(1, n)]
    there = jax.ShapeDtypeStruct(field_values.shape, field_values.dtype)
    pieces = PIECES if nj % PIECES == 0 else 1
    size = nj * ni * nk * levels
    anomaly, field_end = pl.pallas_call(
        write_out,
        out_shape=(there, there),
        in_specs=[near] * 2,
        out_specs=(anywhere, anywhere),
        scratch_shapes=[pltpu.SemaphoreType.DMA((2, pieces))],
        compiler_params=pltpu.CompilerParams(vmem_limit_bytes=1024 * 1024),
        cost_estimate=pl.CostEstimate(flops=0, bytes_accessed=16 * size, transcendentals=0),
        name="write_out",
    )(scaled, last)
    anomaly = pl.pallas_call(
        write_late,
        out_shape=there,
        in_specs=[anywhere] + [near] * (2 + len(others)),
        out_specs=anywhere,
        input_output_aliases={0: 0},
        scratch_shapes=[pltpu.VMEM((outer, nj) + small[2:], jnp.float32), pltpu.SemaphoreType.DMA((outer,))],
        compiler_params=pltpu.CompilerParams(vmem_limit_bytes=2 * 1024 * 1024),
        name="write_late",
    )(anomaly, last, late, *others)
    return anomaly, field_end


def solution(mesh):
    spec = P(("trial", "rows"), "cols", "slabs", None)
    return jax.shard_map(
        on_device, mesh=mesh, in_specs=(spec,) * 3, out_specs=(spec, spec), check_vma=False
    )
```

```python
import functools

import jax
import jax.numpy as jnp
from jax import lax
from jax.experimental import pallas as pl
from jax.experimental.pallas import tpu as pltpu
from jax.sharding import PartitionSpec as P

STEPS = 4
TILE = 8
PIECES = 4
FINE = (4,)
YIELD = 1
PAUSE = 2000
MESH = pl.DeviceIdType.MESH


def kernel(
    sizes, coarse, parts, field, conductance, source, scaled, last, late,
    u, cond, src, own, others,
    load_sem, send_sem, recv_sem, jsend_sem, jrecv_sem, ksend_sem, krecv_sem, ssend_sem, srecv_sem,
):
    rows, cols, slabs = sizes
    nj, ni, nk, _ = field.shape
    row, col, slab = (lax.axis_index(name) for name in ("rows", "cols", "slabs"))
    has = {
        "i-": col > 0, "i+": col < cols - 1,
        "j-": row > 0, "j+": row < rows - 1,
        "k-": slab > 0, "k+": slab < slabs - 1,
    }
    to = {
        "i-": {"cols": jnp.maximum(col - 1, 0)}, "i+": {"cols": jnp.minimum(col + 1, cols - 1)},
        "j-": {"rows": jnp.maximum(row - 1, 0)}, "j+": {"rows": jnp.minimum(row + 1, rows - 1)},
        "k-": {"slabs": jnp.maximum(slab - 1, 0)}, "k+": {"slabs": jnp.minimum(slab + 1, slabs - 1)},
    }
    opposite = {"i-": "i+", "i+": "i-", "j-": "j+", "j+": "j-", "k-": "k+", "k+": "k-"}
    first_core = lax.rem(lax.axis_index("trial"), 2) == 0
    descending = lax.rem(slab, 2) == 0

    def start_of(of, n):
        before, size = sum(of[:n]), of[n]
        return pl.multiple_of(jnp.where(descending, nk - before - size, before), TILE)

    outer, inner = planes_of(ni)

    def load(planes, ks, sem):
        inside = pl.ds(ks.start + TILE, ks.size)
        return pltpu.make_async_copy(
            field.at[:, pl.ds(planes[0], len(planes)), ks],
            u.at[0, pl.ds(1, nj), pl.ds(planes[0] + 1, len(planes)), inside], load_sem.at[sem],
        )

    early = [
        [load((i,), pl.ds(start_of(coarse, n), coarse[n]), n * len(outer) + p) for p, i in enumerate(outer)]
        for n in range(len(coarse))
    ]
    used = len(coarse) * len(outer)
    loads = [
        pltpu.make_async_copy(conductance, cond, load_sem.at[used]),
        pltpu.make_async_copy(source, src, load_sem.at[used + 1]),
    ]
    rest = [load(inner, pl.ds(0, nk), used + 2)] if inner else []
    for part in early:
        for copy in part:
            copy.start()

    barrier = pltpu.get_barrier_semaphore()
    expected = rows - 1
    for off in range(1, rows):
        pl.semaphore_signal(barrier, inc=1, device_id={"rows": lax.rem(row + off, rows)}, device_id_type=MESH)
    for side in ("i-", "i+", "k-", "k+"):
        expected = expected + jnp.where(has[side], 1, 0)

        @pl.when(has[side])
        def _():
            pl.semaphore_signal(barrier, inc=1, device_id=to[side], device_id_type=MESH)

    pl.semaphore_wait(barrier, expected)

    def edges_of(n):
        first, final = n == 0, n == len(coarse) - 1
        low = jnp.where(descending, final, first)
        high = jnp.where(descending, first, final)
        return low, high

    def face(side, t, n, first):
        of = parts[t] if side[0] == "i" else coarse
        k0, kq = start_of(of, n), of[n]
        inside = pl.ds(pl.multiple_of(TILE + k0, TILE), kq)
        js, is_ = pl.ds(1, nj), pl.ds(1, ni)
        if side[0] == "i":
            here, there = (1, ni + 1) if side == "i-" else (ni, 0)
            dst = u.at[t, js, there, inside]
            start = u.at[t, js, here, inside]
        else:
            here, there = (1, nj + 1) if side == "j-" else (nj, 0)
            dst = u.at[t, there, is_, inside]
            start = field.at[here - 1, :, pl.ds(k0, kq)] if first else u.at[t, here, is_, inside]
        d = 0 if side[1] == "-" else 1
        sent, received = (send_sem, recv_sem) if side[0] == "i" else (jsend_sem, jrecv_sem)
        return pltpu.make_async_remote_copy(
            src_ref=start, dst_ref=dst, send_sem=sent.at[d, t, n], recv_sem=received.at[d, t, n],
            device_id=to[side], device_id_type=MESH,
        )

    def kface(side, t, first):
        js, is_ = pl.ds(1, nj), pl.ds(1, ni)
        here, there = (TILE, TILE + nk) if side == "k-" else (nk, 0)
        start = field.at[:, :, pl.ds(here - TILE, TILE)] if first else u.at[t, js, is_, pl.ds(here, TILE)]
        d = 0 if side == "k-" else 1
        return pltpu.make_async_remote_copy(
            src_ref=start, dst_ref=u.at[t, js, is_, pl.ds(there, TILE)],
            send_sem=ksend_sem.at[d, t], recv_sem=krecv_sem.at[d, t],
            device_id=to[side], device_id_type=MESH,
        )

    def fine_of(t, n):
        low, done = sum(coarse[:n]), sum(coarse[:n + 1])
        return [m for m in range(len(parts[t])) if low <= sum(parts[t][:m]) < done]

    def send_i(t, n):
        for side in ("i-", "i+"):
            @pl.when(has[side])
            def _():
                for m in fine_of(t, n):
                    face(side, t, m, False).start()

    def send_others(t, n, first):
        for side in ("j-", "j+"):
            @pl.when(has[side])
            def _():
                face(side, t, n, first).start()

        low, high = edges_of(n)

        @pl.when(low & has["k-"])
        def _():
            kface("k-", t, first).start()

        @pl.when(high & has["k+"])
        def _():
            kface("k+", t, first).start()

    def wait_i(t, n):
        for side in ("i-", "i+"):
            @pl.when(has[opposite[side]])
            def _():
                face(side, t, n, False).wait_recv()

    def wait_others(t, n):
        for side in ("j-", "j+"):
            @pl.when(has[opposite[side]])
            def _():
                face(side, t, n, False).wait_recv()

        low, high = edges_of(n)

        @pl.when(high & has["k+"])
        def _():
            kface("k-", t, False).wait_recv()

        @pl.when(low & has["k-"])
        def _():
            kface("k+", t, False).wait_recv()

    def wait_sent_i(t, who):
        for side in ("i-", "i+"):
            @pl.when(who & has[side])
            def _():
                for n in range(len(parts[t])):
                    face(side, t, n, False).wait_send()

    def wait_sent(t):
        wait_sent_i(t, first_core if t == YIELD else True)
        for side in ("j-", "j+"):
            @pl.when(has[side])
            def _():
                for n in range(len(coarse)):
                    face(side, t, n, False).wait_send()

        for side in ("k-", "k+"):
            @pl.when(has[side])
            def _():
                kface(side, t, False).wait_send()

    for n in range(len(coarse)):
        for copy in early[n]:
            copy.wait()
        send_i(0, n)
    for n in range(len(coarse)):
        send_others(0, n, True)
    for copy in rest:
        copy.start()
    for copy in loads:
        copy.start()

    def zero_plane(t, j, i):
        u[t, j, i, pl.ds(TILE, nk)] = jnp.zeros((nk, u.shape[-1]), u.dtype)

    @pl.loop(0, STEPS)
    def _(t):
        for side, i in (("i-", 0), ("i+", ni + 1)):
            @pl.when(jnp.logical_not(has[side]))
            def _():
                @pl.loop(0, nj)
                def _(j):
                    zero_plane(t, j + 1, i)

        for side, j in (("j-", 0), ("j+", nj + 1)):
            @pl.when(jnp.logical_not(has[side]))
            def _():
                for i in range(ni):
                    zero_plane(t, j, i + 1)

        for side, k in (("k-", 0), ("k+", TILE + nk)):
            @pl.when(jnp.logical_not(has[side]))
            def _():
                @pl.loop(0, nj)
                def _(j):
                    for i in range(ni):
                        u[t, j + 1, i + 1, pl.ds(k, TILE)] = jnp.zeros((TILE, u.shape[-1]), u.dtype)

    for copy in rest + loads:
        copy.wait()

    def stencil(t, j, i, k0, kq, skip=(False, False)):
        inner = pl.ds(pl.multiple_of(TILE + k0, TILE), kq)
        tall = u[t, j + 1, i + 1, pl.ds(k0, kq + 2 * TILE)]
        middle = tall[TILE:TILE + kq]
        spread = u[t, j, i + 1, inner] + u[t, j + 2, i + 1, inner]
        for beside, left_out in ((i, skip[0]), (i + 2, skip[1])):
            if not left_out:
                spread = spread + u[t, j + 1, beside, inner]
        spread = spread + tall[TILE - 1:TILE - 1 + kq] + tall[TILE + 1:TILE + 1 + kq]
        spread = spread - 6.0 * middle
        own_k = pl.ds(k0, kq)
        return middle + cond[j, i, own_k] * spread + src[j, i, own_k]

    def middle_step(t, n):
        k0, kq = start_of(coarse, n), coarse[n]
        for m in fine_of(t, n):
            wait_i(t, m)
        wait_others(t, n)

        @pl.loop(0, nj)
        def _(jj):
            j = lax.rem(jj + nj - 1, nj)
            for i in range(ni):
                u[t + 1, j + 1, i + 1, pl.ds(pl.multiple_of(TILE + k0, TILE), kq)] = stencil(t, j, i, k0, kq)

        if t == YIELD and n == 0:
            wait_sent_i(t, jnp.logical_not(first_core))

            @pl.when(jnp.logical_not(first_core))
            def _():
                pl.delay(PAUSE)

        send_i(t + 1, n)
        send_others(t + 1, n, False)

    for t in range(STEPS - 1):
        for n in range(len(coarse)):
            middle_step(t, n)
        if t > 0:
            wait_sent(t - 1)

    t = STEPS - 1
    final = parts[t]
    groups = [(inner, len(outer), coarse, n, n) for n in range(len(coarse))] if inner else []
    groups += [(outer, 0, final, n, len(coarse) + n) for n in range(len(final) - 1)]

    def stats_copy(off, group):
        planes, at, of, n, sem = group
        place = (slice(None), pl.ds(at, len(planes)), pl.ds(start_of(of, n), of[n]))
        return pltpu.make_async_remote_copy(
            src_ref=own.at[place], dst_ref=others.at[(off - 1,) + place],
            send_sem=ssend_sem.at[off - 1, sem], recv_sem=srecv_sem.at[off - 1, sem],
            device_id={"rows": lax.rem(row + off, rows)}, device_id_type=MESH,
        )

    def blocks(of, n):
        def wrap(body):
            k0 = start_of(of, n)

            @pl.loop(0, of[n] // TILE)
            def _(b):
                body(pl.multiple_of(k0 + b * TILE, TILE), pl.multiple_of(b * TILE, TILE))
        return wrap

    def sums_of(news):
        mean = sum(news[1:], news[0]) / nj
        aways = [new - mean for new in news]
        squares = [away * away for away in aways]
        return mean, sum(squares[1:], squares[0])

    def inner_step(group):
        planes, at, of, n, _ = group

        @blocks(of, n)
        def _(k, b):
            ks = pl.ds(k, TILE)
            for p, i in enumerate(planes):
                news = [stencil(t, j, i, k, TILE) for j in range(nj)]
                own[0, at + p, ks], own[1, at + p, ks] = sums_of(news)
                for j in range(nj):
                    last[j, i, ks] = news[j]

        for off in range(1, rows):
            stats_copy(off, group).start()

    def outer_ahead(n):
        @blocks(coarse, n)
        def _(k, b):
            for i in outer:
                for j in range(nj):
                    last[j, i, pl.ds(k, TILE)] = stencil(t, j, i, k, TILE, skip=(i == 0, i == ni - 1))

    def outer_step(n, into):
        @blocks(final, n)
        def _(k, b):
            ks, inside = pl.ds(k, TILE), pl.ds(pl.multiple_of(TILE + k, TILE), TILE)
            for p, i in enumerate(outer):
                faces = [face for face, here in ((0, i == 0), (ni + 1, i == ni - 1)) if here]
                news = []
                for j in range(nj):
                    arrived = [u[t, j + 1, face, inside] for face in faces]
                    news.append(last[j, i, ks] + cond[j, i, ks] * sum(arrived[1:], arrived[0]))
                if into is own:
                    own[0, p, ks], own[1, p, ks] = sums_of(news)
                else:
                    into[0, p, pl.ds(b, TILE)], into[1, p, pl.ds(b, TILE)] = sums_of(news)
                for j in range(nj):
                    last[j, i, ks] = news[j]

    def finish(group):
        planes, at, of, n, _ = group
        for off in range(1, rows):
            stats_copy(off, group).wait_recv()

        @blocks(of, n)
        def _(k, b):
            ks = pl.ds(k, TILE)
            for p, i in enumerate(planes):
                means = [own[0, at + p, ks]] + [others[off - 1, 0, at + p, ks] for off in range(1, rows)]
                spreads = [own[1, at + p, ks]] + [others[off - 1, 1, at + p, ks] for off in range(1, rows)]
                mean, scale = joined(nj, means, spreads)
                for j in range(nj):
                    scaled[j, i, ks] = (last[j, i, ks] - mean) * scale

    for n in range(len(coarse)):
        wait_others(t, n)
    count = len(coarse) if inner else 0
    for group in groups[:count]:
        inner_step(group)
    for n in range(len(coarse)):
        outer_ahead(n)
    for group in groups[:count]:
        finish(group)
    wait_sent(STEPS - 2)
    for n in range(len(final) - 1):
        wait_i(t, n)
        outer_step(n, own)
        for off in range(1, rows):
            stats_copy(off, groups[count + n]).start()
        if n > 0:
            finish(groups[count + n - 1])
    wait_i(t, len(final) - 1)
    outer_step(len(final) - 1, late)
    if len(final) > 1:
        finish(groups[-1])
    for group in groups:
        for off in range(1, rows):
            stats_copy(off, group).wait_send()
    wait_sent(t)


def planes_of(ni):
    outer = tuple(range(ni)) if ni < 3 else (0, ni - 1)
    return outer, tuple(i for i in range(ni) if i not in outer)


def joined(nj, means, spreads):
    count = len(means)
    mean = sum(means[1:], means[0]) / count
    spread = sum(spreads[1:], spreads[0])
    for other in means:
        spread = spread + nj * ((other - mean) * (other - mean))
    return mean, lax.rsqrt(spread / (nj * count) + 0.0001)


def write_out(near_anomaly, near_field, anomaly, field_end, sems):
    copies = []
    for which, (start, dst) in enumerate(((near_field, field_end), (near_anomaly, anomaly))):
        pieces = sems.shape[1]
        depth = start.shape[0] // pieces
        for piece in range(pieces):
            js = pl.ds(piece * depth, depth)
            copies.append(pltpu.make_async_copy(start.at[js], dst.at[js], sems.at[which, piece]))
    for copy in copies:
        copy.start()
    for copy in copies:
        copy.wait()


def write_late(before, near_field, late, *refs):
    others, (anomaly, scaled, sems) = refs[:-3], refs[-3:]
    nj, ni, nk, _ = near_field.shape
    size = late.shape[2]
    descending = lax.rem(lax.axis_index("slabs"), 2) == 0
    start = pl.multiple_of(jnp.where(descending, 0, nk - size), TILE)
    copies = []
    for p, i in enumerate(planes_of(ni)[0]):
        @pl.loop(0, size // TILE)
        def _(b):
            ks = pl.ds(pl.multiple_of(b * TILE, TILE), TILE)
            ms = pl.ds(pl.multiple_of(start + b * TILE, TILE), TILE)
            stats = (late,) + others
            mean, scale = joined(nj, [of[0, p, ks] for of in stats], [of[1, p, ks] for of in stats])
            for j in range(nj):
                scaled[p, j, ks] = (near_field[j, i, ms] - mean) * scale

        copies.append(pltpu.make_async_copy(scaled.at[p], anomaly.at[:, i, pl.ds(start, size)], sems.at[p]))
        copies[-1].start()
    for copy in copies:
        copy.wait()


def parts_of(nk):
    half = nk // 2 if nk % (2 * TILE) == 0 else nk
    coarse = (half,) * (nk // half)
    fine, left = [], half
    for eighths in FINE:
        size = half * eighths // 8 // TILE * TILE
        if 0 < size < left:
            fine.append(size)
            left -= size
    return coarse, (coarse,) * (STEPS - 1) + (coarse[:-1] + tuple(fine) + (left,),)


def on_device(field_values, conductance, source):
    sizes = tuple(lax.axis_size(name) for name in ("rows", "cols", "slabs"))
    nj, ni, nk, levels = field_values.shape
    coarse, parts = parts_of(nk)
    most = max(len(of) for of in parts)
    groups = len(parts[-1]) + len(coarse)
    peers = max(sizes[0] - 1, 1)
    whole = pltpu.VMEM(field_values.shape, field_values.dtype)
    near = pl.BlockSpec(memory_space=pltpu.VMEM)
    outer = len(planes_of(ni)[0])
    small = (2, outer, parts[-1][-1], levels)
    anywhere = pl.BlockSpec(memory_space=pl.ANY)
    scaled, last, late = pl.pallas_call(
        functools.partial(kernel, sizes, coarse, parts),
        out_shape=(whole, whole, pltpu.VMEM(small, jnp.float32)),
        in_specs=[anywhere] * 3,
        out_specs=(near, near, near),
        scratch_shapes=[
            pltpu.VMEM((STEPS, nj + 2, ni + 2, nk + 2 * TILE, levels), jnp.float32),
            pltpu.VMEM((nj, ni, nk, levels), jnp.float32),
            pltpu.VMEM((nj, ni, nk, levels), jnp.float32),
            pltpu.VMEM((2, ni, nk, levels), jnp.float32),
            pltpu.VMEM((peers, 2, ni, nk, levels), jnp.float32),
            pltpu.SemaphoreType.DMA((len(coarse) * outer + 3,)),
            pltpu.SemaphoreType.DMA((2, STEPS, most)),
            pltpu.SemaphoreType.DMA((2, STEPS, most)),
            pltpu.SemaphoreType.DMA((2, STEPS, len(coarse))),
            pltpu.SemaphoreType.DMA((2, STEPS, len(coarse))),
            pltpu.SemaphoreType.DMA((2, STEPS)),
            pltpu.SemaphoreType.DMA((2, STEPS)),
            pltpu.SemaphoreType.DMA((peers, groups)),
            pltpu.SemaphoreType.DMA((peers, groups)),
        ],
        compiler_params=pltpu.CompilerParams(
            collective_id=0, has_side_effects=True, vmem_limit_bytes=52 * 1024 * 1024
        ),
        name="heat_steps",
    )(field_values, conductance, source)
    n = sizes[0]
    others = [lax.ppermute(late, "rows", [(r, (r + off) % n) for r in range(n)]) for off in range(1, n)]
    there = jax.ShapeDtypeStruct(field_values.shape, field_values.dtype)
    pieces = PIECES if nj % PIECES == 0 else 1
    size = nj * ni * nk * levels
    anomaly, field_end = pl.pallas_call(
        write_out,
        out_shape=(there, there),
        in_specs=[near] * 2,
        out_specs=(anywhere, anywhere),
        scratch_shapes=[pltpu.SemaphoreType.DMA((2, pieces))],
        compiler_params=pltpu.CompilerParams(vmem_limit_bytes=1024 * 1024),
        cost_estimate=pl.CostEstimate(flops=0, bytes_accessed=16 * size, transcendentals=0),
        name="write_out",
    )(scaled, last)
    anomaly = pl.pallas_call(
        write_late,
        out_shape=there,
        in_specs=[anywhere] + [near] * (2 + len(others)),
        out_specs=anywhere,
        input_output_aliases={0: 0},
        scratch_shapes=[pltpu.VMEM((outer, nj) + small[2:], jnp.float32), pltpu.SemaphoreType.DMA((outer,))],
        compiler_params=pltpu.CompilerParams(vmem_limit_bytes=2 * 1024 * 1024),
        name="write_late",
    )(anomaly, last, late, *others)
    return anomaly, field_end


def solution(mesh):
    spec = P(("trial", "rows"), "cols", "slabs", None)
    return jax.shard_map(
        on_device, mesh=mesh, in_specs=(spec,) * 3, out_specs=(spec, spec), check_vma=False
    )
```

```python
import functools

import jax
import jax.numpy as jnp
from jax import lax
from jax.experimental import pallas as pl
from jax.experimental.pallas import tpu as pltpu
from jax.sharding import PartitionSpec as P

STEPS = 4
TILE = 8
PIECES = 4
FINE = (4,)
YIELD = 1
PAUSE = 1000
MESH = pl.DeviceIdType.MESH


def kernel(
    sizes, coarse, parts, field, conductance, source, scaled, last, late,
    u, cond, src, own, others,
    load_sem, send_sem, recv_sem, jsend_sem, jrecv_sem, ksend_sem, krecv_sem, ssend_sem, srecv_sem, ready_sem,
):
    rows, cols, slabs = sizes
    nj, ni, nk, _ = field.shape
    row, col, slab = (lax.axis_index(name) for name in ("rows", "cols", "slabs"))
    has = {
        "i-": col > 0, "i+": col < cols - 1,
        "j-": row > 0, "j+": row < rows - 1,
        "k-": slab > 0, "k+": slab < slabs - 1,
    }
    to = {
        "i-": {"cols": jnp.maximum(col - 1, 0)}, "i+": {"cols": jnp.minimum(col + 1, cols - 1)},
        "j-": {"rows": jnp.maximum(row - 1, 0)}, "j+": {"rows": jnp.minimum(row + 1, rows - 1)},
        "k-": {"slabs": jnp.maximum(slab - 1, 0)}, "k+": {"slabs": jnp.minimum(slab + 1, slabs - 1)},
    }
    opposite = {"i-": "i+", "i+": "i-", "j-": "j+", "j+": "j-", "k-": "k+", "k+": "k-"}
    first_core = lax.rem(lax.axis_index("trial"), 2) == 0
    descending = lax.rem(slab, 2) == 0

    def start_of(of, n):
        before, size = sum(of[:n]), of[n]
        return pl.multiple_of(jnp.where(descending, nk - before - size, before), TILE)

    outer, inner = planes_of(ni)
    loads = [
        pltpu.make_async_copy(field, u.at[0, pl.ds(1, nj), pl.ds(1, ni), pl.ds(TILE, nk)], load_sem.at[0]),
        pltpu.make_async_copy(conductance, cond, load_sem.at[1]),
        pltpu.make_async_copy(source, src, load_sem.at[2]),
    ]

    barrier = pltpu.get_barrier_semaphore()
    for off in range(1, rows):
        @pl.when(row + off < rows)
        def _():
            pl.semaphore_signal(barrier, inc=1, device_id={"rows": jnp.minimum(row + off, rows - 1)}, device_id_type=MESH)

    expected = row
    for side in ("i", "k"):
        expected = expected + jnp.where(has[side + "-"], 1, 0)

        @pl.when(has[side + "+"])
        def _():
            pl.semaphore_signal(barrier, inc=1, device_id=to[side + "+"], device_id_type=MESH)


    @pl.when(expected > 0)
    def _():
        pl.semaphore_wait(barrier, expected)

    for side, at in (("i", rows - 1), ("k", rows)):
        @pl.when(has[side + "-"])
        def _():
            pl.semaphore_signal(ready_sem.at[at], inc=1, device_id=to[side + "-"], device_id_type=MESH)

    for off in range(1, rows):
        @pl.when(row >= off)
        def _():
            pl.semaphore_signal(
                ready_sem.at[off - 1], inc=1, device_id={"rows": jnp.maximum(row - off, 0)}, device_id_type=MESH
            )

    def edges_of(n):
        first, final = n == 0, n == len(coarse) - 1
        low = jnp.where(descending, final, first)
        high = jnp.where(descending, first, final)
        return low, high

    def face(side, t, n, first):
        of = parts[t] if side[0] == "i" else coarse
        k0, kq = start_of(of, n), of[n]
        inside = pl.ds(pl.multiple_of(TILE + k0, TILE), kq)
        js, is_ = pl.ds(1, nj), pl.ds(1, ni)
        if side[0] == "i":
            here, there = (1, ni + 1) if side == "i-" else (ni, 0)
            dst = u.at[t, js, there, inside]
            start = field.at[:, here - 1, pl.ds(k0, kq)] if first else u.at[t, js, here, inside]
        else:
            here, there = (1, nj + 1) if side == "j-" else (nj, 0)
            dst = u.at[t, there, is_, inside]
            start = field.at[here - 1, :, pl.ds(k0, kq)] if first else u.at[t, here, is_, inside]
        d = 0 if side[1] == "-" else 1
        sent, received = (send_sem, recv_sem) if side[0] == "i" else (jsend_sem, jrecv_sem)
        return pltpu.make_async_remote_copy(
            src_ref=start, dst_ref=dst, send_sem=sent.at[d, t, n], recv_sem=received.at[d, t, n],
            device_id=to[side], device_id_type=MESH,
        )

    def kface(side, t, first):
        js, is_ = pl.ds(1, nj), pl.ds(1, ni)
        here, there = (TILE, TILE + nk) if side == "k-" else (nk, 0)
        start = field.at[:, :, pl.ds(here - TILE, TILE)] if first else u.at[t, js, is_, pl.ds(here, TILE)]
        d = 0 if side == "k-" else 1
        return pltpu.make_async_remote_copy(
            src_ref=start, dst_ref=u.at[t, js, is_, pl.ds(there, TILE)],
            send_sem=ksend_sem.at[d, t], recv_sem=krecv_sem.at[d, t],
            device_id=to[side], device_id_type=MESH,
        )

    def fine_of(t, n):
        low, done = sum(coarse[:n]), sum(coarse[:n + 1])
        return [m for m in range(len(parts[t])) if low <= sum(parts[t][:m]) < done]

    def send_i(t, n, first, towards=("i-", "i+")):
        for side in towards:
            @pl.when(has[side])
            def _():
                for m in fine_of(t, n):
                    face(side, t, m, first).start()

    def send_others(t, n, first):
        for side in ("j-", "j+"):
            @pl.when(has[side])
            def _():
                face(side, t, n, first).start()

        low, high = edges_of(n)

        @pl.when(low & has["k-"])
        def _():
            kface("k-", t, first).start()

        @pl.when(high & has["k+"])
        def _():
            kface("k+", t, first).start()

    def wait_i(t, n):
        for side in ("i-", "i+"):
            @pl.when(has[opposite[side]])
            def _():
                face(side, t, n, False).wait_recv()

    def wait_others(t, n):
        for side in ("j-", "j+"):
            @pl.when(has[opposite[side]])
            def _():
                face(side, t, n, False).wait_recv()

        low, high = edges_of(n)

        @pl.when(high & has["k+"])
        def _():
            kface("k-", t, False).wait_recv()

        @pl.when(low & has["k-"])
        def _():
            kface("k+", t, False).wait_recv()

    def wait_sent_i(t, who):
        for side in ("i-", "i+"):
            @pl.when(who & has[side])
            def _():
                for n in range(len(parts[t])):
                    face(side, t, n, False).wait_send()

    def wait_sent(t):
        wait_sent_i(t, first_core if t == YIELD else True)
        for side in ("j-", "j+"):
            @pl.when(has[side])
            def _():
                for n in range(len(coarse)):
                    face(side, t, n, False).wait_send()

        for side in ("k-", "k+"):
            @pl.when(has[side])
            def _():
                kface(side, t, False).wait_send()

    for n in range(len(coarse)):
        send_i(0, n, True, ("i-",))

    @pl.when(has["i+"])
    def _():
        pl.semaphore_wait(ready_sem.at[rows - 1], 1)

    for n in range(len(coarse)):
        send_i(0, n, True, ("i+",))

    @pl.when(has["k+"])
    def _():
        pl.semaphore_wait(ready_sem.at[rows], 1)

    for off in range(1, rows):
        @pl.when(row + off < rows)
        def _():
            pl.semaphore_wait(ready_sem.at[off - 1], 1)

    for n in range(len(coarse)):
        send_others(0, n, True)
    for copy in loads:
        copy.start()

    def zero_plane(t, j, i):
        u[t, j, i, pl.ds(TILE, nk)] = jnp.zeros((nk, u.shape[-1]), u.dtype)

    @pl.loop(0, STEPS)
    def _(t):
        for side, i in (("i-", 0), ("i+", ni + 1)):
            @pl.when(jnp.logical_not(has[side]))
            def _():
                @pl.loop(0, nj)
                def _(j):
                    zero_plane(t, j + 1, i)

        for side, j in (("j-", 0), ("j+", nj + 1)):
            @pl.when(jnp.logical_not(has[side]))
            def _():
                for i in range(ni):
                    zero_plane(t, j, i + 1)

        for side, k in (("k-", 0), ("k+", TILE + nk)):
            @pl.when(jnp.logical_not(has[side]))
            def _():
                @pl.loop(0, nj)
                def _(j):
                    for i in range(ni):
                        u[t, j + 1, i + 1, pl.ds(k, TILE)] = jnp.zeros((TILE, u.shape[-1]), u.dtype)

    for copy in loads:
        copy.wait()

    def stencil(t, j, i, k0, kq, skip=(False, False)):
        inner = pl.ds(pl.multiple_of(TILE + k0, TILE), kq)
        tall = u[t, j + 1, i + 1, pl.ds(k0, kq + 2 * TILE)]
        middle = tall[TILE:TILE + kq]
        spread = u[t, j, i + 1, inner] + u[t, j + 2, i + 1, inner]
        for beside, left_out in ((i, skip[0]), (i + 2, skip[1])):
            if not left_out:
                spread = spread + u[t, j + 1, beside, inner]
        spread = spread + tall[TILE - 1:TILE - 1 + kq] + tall[TILE + 1:TILE + 1 + kq]
        spread = spread - 6.0 * middle
        own_k = pl.ds(k0, kq)
        return middle + cond[j, i, own_k] * spread + src[j, i, own_k]

    def middle_step(t, n):
        k0, kq = start_of(coarse, n), coarse[n]
        for m in fine_of(t, n):
            wait_i(t, m)
        wait_others(t, n)

        @pl.loop(0, nj)
        def _(jj):
            j = lax.rem(jj + nj - 1, nj)
            for i in range(ni):
                u[t + 1, j + 1, i + 1, pl.ds(pl.multiple_of(TILE + k0, TILE), kq)] = stencil(t, j, i, k0, kq)

        if t == YIELD and n == 0:
            wait_sent_i(t, jnp.logical_not(first_core))

            @pl.when(jnp.logical_not(first_core))
            def _():
                pl.delay(PAUSE)

        send_i(t + 1, n, False)
        send_others(t + 1, n, False)

    for t in range(STEPS - 1):
        for n in range(len(coarse)):
            middle_step(t, n)
        if t > 0:
            wait_sent(t - 1)

    t = STEPS - 1
    final = parts[t]
    groups = [(inner, len(outer), coarse, n, n) for n in range(len(coarse))] if inner else []
    groups += [(outer, 0, final, n, len(coarse) + n) for n in range(len(final) - 1)]

    def stats_copy(off, group):
        planes, at, of, n, sem = group
        place = (slice(None), pl.ds(at, len(planes)), pl.ds(start_of(of, n), of[n]))
        return pltpu.make_async_remote_copy(
            src_ref=own.at[place], dst_ref=others.at[(off - 1,) + place],
            send_sem=ssend_sem.at[off - 1, sem], recv_sem=srecv_sem.at[off - 1, sem],
            device_id={"rows": lax.rem(row + off, rows)}, device_id_type=MESH,
        )

    def blocks(of, n):
        def wrap(body):
            k0 = start_of(of, n)

            @pl.loop(0, of[n] // TILE)
            def _(b):
                body(pl.multiple_of(k0 + b * TILE, TILE), pl.multiple_of(b * TILE, TILE))
        return wrap

    def sums_of(news):
        mean = sum(news[1:], news[0]) / nj
        aways = [new - mean for new in news]
        squares = [away * away for away in aways]
        return mean, sum(squares[1:], squares[0])

    def inner_step(group):
        planes, at, of, n, _ = group

        @blocks(of, n)
        def _(k, b):
            ks = pl.ds(k, TILE)
            for p, i in enumerate(planes):
                news = [stencil(t, j, i, k, TILE) for j in range(nj)]
                own[0, at + p, ks], own[1, at + p, ks] = sums_of(news)
                for j in range(nj):
                    last[j, i, ks] = news[j]

        for off in range(1, rows):
            stats_copy(off, group).start()

    def outer_ahead(n):
        @blocks(coarse, n)
        def _(k, b):
            for i in outer:
                for j in range(nj):
                    last[j, i, pl.ds(k, TILE)] = stencil(t, j, i, k, TILE, skip=(i == 0, i == ni - 1))

    def outer_step(n, into):
        @blocks(final, n)
        def _(k, b):
            ks, inside = pl.ds(k, TILE), pl.ds(pl.multiple_of(TILE + k, TILE), TILE)
            for p, i in enumerate(outer):
                faces = [face for face, here in ((0, i == 0), (ni + 1, i == ni - 1)) if here]
                news = []
                for j in range(nj):
                    arrived = [u[t, j + 1, face, inside] for face in faces]
                    news.append(last[j, i, ks] + cond[j, i, ks] * sum(arrived[1:], arrived[0]))
                if into is own:
                    own[0, p, ks], own[1, p, ks] = sums_of(news)
                else:
                    into[0, p, pl.ds(b, TILE)], into[1, p, pl.ds(b, TILE)] = sums_of(news)
                for j in range(nj):
                    last[j, i, ks] = news[j]

    def finish(group):
        planes, at, of, n, _ = group
        for off in range(1, rows):
            stats_copy(off, group).wait_recv()

        @blocks(of, n)
        def _(k, b):
            ks = pl.ds(k, TILE)
            for p, i in enumerate(planes):
                means = [own[0, at + p, ks]] + [others[off - 1, 0, at + p, ks] for off in range(1, rows)]
                spreads = [own[1, at + p, ks]] + [others[off - 1, 1, at + p, ks] for off in range(1, rows)]
                mean, scale = joined(nj, means, spreads)
                for j in range(nj):
                    scaled[j, i, ks] = (last[j, i, ks] - mean) * scale

    for n in range(len(coarse)):
        wait_others(t, n)
    count = len(coarse) if inner else 0
    for group in groups[:count]:
        inner_step(group)
    for n in range(len(coarse)):
        outer_ahead(n)
    for group in groups[:count]:
        finish(group)
    wait_sent(STEPS - 2)
    for n in range(len(final) - 1):
        wait_i(t, n)
        outer_step(n, own)
        for off in range(1, rows):
            stats_copy(off, groups[count + n]).start()
        if n > 0:
            finish(groups[count + n - 1])
    wait_i(t, len(final) - 1)
    outer_step(len(final) - 1, late)
    if len(final) > 1:
        finish(groups[-1])
    for group in groups:
        for off in range(1, rows):
            stats_copy(off, group).wait_send()
    wait_sent(t)


def planes_of(ni):
    outer = tuple(range(ni)) if ni < 3 else (0, ni - 1)
    return outer, tuple(i for i in range(ni) if i not in outer)


def joined(nj, means, spreads):
    count = len(means)
    mean = sum(means[1:], means[0]) / count
    spread = sum(spreads[1:], spreads[0])
    for other in means:
        spread = spread + nj * ((other - mean) * (other - mean))
    return mean, lax.rsqrt(spread / (nj * count) + 0.0001)


def write_out(near_anomaly, near_field, anomaly, field_end, sems):
    copies = []
    for which, (start, dst) in enumerate(((near_field, field_end), (near_anomaly, anomaly))):
        pieces = sems.shape[1]
        depth = start.shape[0] // pieces
        for piece in range(pieces):
            js = pl.ds(piece * depth, depth)
            copies.append(pltpu.make_async_copy(start.at[js], dst.at[js], sems.at[which, piece]))
    for copy in copies:
        copy.start()
    for copy in copies:
        copy.wait()


def write_late(before, near_field, late, *refs):
    others, (anomaly, scaled, sems) = refs[:-3], refs[-3:]
    nj, ni, nk, _ = near_field.shape
    size = late.shape[2]
    descending = lax.rem(lax.axis_index("slabs"), 2) == 0
    start = pl.multiple_of(jnp.where(descending, 0, nk - size), TILE)
    copies = []
    for p, i in enumerate(planes_of(ni)[0]):
        @pl.loop(0, size // TILE)
        def _(b):
            ks = pl.ds(pl.multiple_of(b * TILE, TILE), TILE)
            ms = pl.ds(pl.multiple_of(start + b * TILE, TILE), TILE)
            stats = (late,) + others
            mean, scale = joined(nj, [of[0, p, ks] for of in stats], [of[1, p, ks] for of in stats])
            for j in range(nj):
                scaled[p, j, ks] = (near_field[j, i, ms] - mean) * scale

        copies.append(pltpu.make_async_copy(scaled.at[p], anomaly.at[:, i, pl.ds(start, size)], sems.at[p]))
        copies[-1].start()
    for copy in copies:
        copy.wait()


def parts_of(nk):
    half = nk // 2 if nk % (2 * TILE) == 0 else nk
    coarse = (half,) * (nk // half)
    fine, left = [], half
    for eighths in FINE:
        size = half * eighths // 8 // TILE * TILE
        if 0 < size < left:
            fine.append(size)
            left -= size
    return coarse, (coarse,) * (STEPS - 1) + (coarse[:-1] + tuple(fine) + (left,),)


def on_device(field_values, conductance, source):
    sizes = tuple(lax.axis_size(name) for name in ("rows", "cols", "slabs"))
    nj, ni, nk, levels = field_values.shape
    coarse, parts = parts_of(nk)
    most = max(len(of) for of in parts)
    groups = len(parts[-1]) + len(coarse)
    peers = max(sizes[0] - 1, 1)
    whole = pltpu.VMEM(field_values.shape, field_values.dtype)
    near = pl.BlockSpec(memory_space=pltpu.VMEM)
    outer = len(planes_of(ni)[0])
    small = (2, outer, parts[-1][-1], levels)
    anywhere = pl.BlockSpec(memory_space=pl.ANY)
    scaled, last, late = pl.pallas_call(
        functools.partial(kernel, sizes, coarse, parts),
        out_shape=(whole, whole, pltpu.VMEM(small, jnp.float32)),
        in_specs=[anywhere] * 3,
        out_specs=(near, near, near),
        scratch_shapes=[
            pltpu.VMEM((STEPS, nj + 2, ni + 2, nk + 2 * TILE, levels), jnp.float32),
            pltpu.VMEM((nj, ni, nk, levels), jnp.float32),
            pltpu.VMEM((nj, ni, nk, levels), jnp.float32),
            pltpu.VMEM((2, ni, nk, levels), jnp.float32),
            pltpu.VMEM((peers, 2, ni, nk, levels), jnp.float32),
            pltpu.SemaphoreType.DMA((3,)),
            pltpu.SemaphoreType.DMA((2, STEPS, most)),
            pltpu.SemaphoreType.DMA((2, STEPS, most)),
            pltpu.SemaphoreType.DMA((2, STEPS, len(coarse))),
            pltpu.SemaphoreType.DMA((2, STEPS, len(coarse))),
            pltpu.SemaphoreType.DMA((2, STEPS)),
            pltpu.SemaphoreType.DMA((2, STEPS)),
            pltpu.SemaphoreType.DMA((peers, groups)),
            pltpu.SemaphoreType.DMA((peers, groups)),
            pltpu.SemaphoreType.REGULAR((sizes[0] + 1,)),
        ],
        compiler_params=pltpu.CompilerParams(
            collective_id=0, has_side_effects=True, vmem_limit_bytes=52 * 1024 * 1024
        ),
        name="heat_steps",
    )(field_values, conductance, source)
    n = sizes[0]
    others = [lax.ppermute(late, "rows", [(r, (r + off) % n) for r in range(n)]) for off in range(1, n)]
    there = jax.ShapeDtypeStruct(field_values.shape, field_values.dtype)
    pieces = PIECES if nj % PIECES == 0 else 1
    size = nj * ni * nk * levels
    anomaly, field_end = pl.pallas_call(
        write_out,
        out_shape=(there, there),
        in_specs=[near] * 2,
        out_specs=(anywhere, anywhere),
        scratch_shapes=[pltpu.SemaphoreType.DMA((2, pieces))],
        compiler_params=pltpu.CompilerParams(vmem_limit_bytes=1024 * 1024),
        cost_estimate=pl.CostEstimate(flops=0, bytes_accessed=16 * size, transcendentals=0),
        name="write_out",
    )(scaled, last)
    anomaly = pl.pallas_call(
        write_late,
        out_shape=there,
        in_specs=[anywhere] + [near] * (2 + len(others)),
        out_specs=anywhere,
        input_output_aliases={0: 0},
        scratch_shapes=[pltpu.VMEM((outer, nj) + small[2:], jnp.float32), pltpu.SemaphoreType.DMA((outer,))],
        compiler_params=pltpu.CompilerParams(vmem_limit_bytes=2 * 1024 * 1024),
        name="write_late",
    )(anomaly, last, late, *others)
    return anomaly, field_end


def solution(mesh):
    spec = P(("trial", "rows"), "cols", "slabs", None)
    return jax.shard_map(
        on_device, mesh=mesh, in_specs=(spec,) * 3, out_specs=(spec, spec), check_vma=False
    )
```

```python
import functools

import jax
import jax.numpy as jnp
from jax import lax
from jax.experimental import pallas as pl
from jax.experimental.pallas import tpu as pltpu
from jax.sharding import PartitionSpec as P

STEPS = 4
TILE = 8
PIECES = 4
FINE = (4,)
YIELD = 1
PAUSE = 1200
MESH = pl.DeviceIdType.MESH


def kernel(
    sizes, coarse, parts, field, conductance, source, scaled, last, late,
    u, cond, src, own, others,
    load_sem, send_sem, recv_sem, jsend_sem, jrecv_sem, ksend_sem, krecv_sem, ssend_sem, srecv_sem, ready_sem,
):
    rows, cols, slabs = sizes
    nj, ni, nk, _ = field.shape
    row, col, slab = (lax.axis_index(name) for name in ("rows", "cols", "slabs"))
    has = {
        "i-": col > 0, "i+": col < cols - 1,
        "j-": row > 0, "j+": row < rows - 1,
        "k-": slab > 0, "k+": slab < slabs - 1,
    }
    to = {
        "i-": {"cols": jnp.maximum(col - 1, 0)}, "i+": {"cols": jnp.minimum(col + 1, cols - 1)},
        "j-": {"rows": jnp.maximum(row - 1, 0)}, "j+": {"rows": jnp.minimum(row + 1, rows - 1)},
        "k-": {"slabs": jnp.maximum(slab - 1, 0)}, "k+": {"slabs": jnp.minimum(slab + 1, slabs - 1)},
    }
    opposite = {"i-": "i+", "i+": "i-", "j-": "j+", "j+": "j-", "k-": "k+", "k+": "k-"}
    first_core = lax.rem(lax.axis_index("trial"), 2) == 0
    descending = lax.rem(slab, 2) == 0

    def start_of(of, n):
        before, size = sum(of[:n]), of[n]
        return pl.multiple_of(jnp.where(descending, nk - before - size, before), TILE)

    outer, inner = planes_of(ni)
    loads = [
        pltpu.make_async_copy(field, u.at[0, pl.ds(1, nj), pl.ds(1, ni), pl.ds(TILE, nk)], load_sem.at[0]),
        pltpu.make_async_copy(conductance, cond, load_sem.at[1]),
        pltpu.make_async_copy(source, src, load_sem.at[2]),
    ]

    barrier = pltpu.get_barrier_semaphore()
    for off in range(1, rows):
        @pl.when(row + off < rows)
        def _():
            pl.semaphore_signal(barrier, inc=1, device_id={"rows": jnp.minimum(row + off, rows - 1)}, device_id_type=MESH)

    expected = row
    for side in ("i", "k"):
        expected = expected + jnp.where(has[side + "-"], 1, 0)

        @pl.when(has[side + "+"])
        def _():
            pl.semaphore_signal(barrier, inc=1, device_id=to[side + "+"], device_id_type=MESH)


    @pl.when(expected > 0)
    def _():
        pl.semaphore_wait(barrier, expected)

    for side, at in (("i", rows - 1), ("k", rows)):
        @pl.when(has[side + "-"])
        def _():
            pl.semaphore_signal(ready_sem.at[at], inc=1, device_id=to[side + "-"], device_id_type=MESH)

    for off in range(1, rows):
        @pl.when(row >= off)
        def _():
            pl.semaphore_signal(
                ready_sem.at[off - 1], inc=1, device_id={"rows": jnp.maximum(row - off, 0)}, device_id_type=MESH
            )

    def edges_of(n):
        first, final = n == 0, n == len(coarse) - 1
        low = jnp.where(descending, final, first)
        high = jnp.where(descending, first, final)
        return low, high

    def face(side, t, n, first):
        of = parts[t] if side[0] == "i" else coarse
        k0, kq = start_of(of, n), of[n]
        inside = pl.ds(pl.multiple_of(TILE + k0, TILE), kq)
        js, is_ = pl.ds(1, nj), pl.ds(1, ni)
        if side[0] == "i":
            here, there = (1, ni + 1) if side == "i-" else (ni, 0)
            dst = u.at[t, js, there, inside]
            start = field.at[:, here - 1, pl.ds(k0, kq)] if first else u.at[t, js, here, inside]
        else:
            here, there = (1, nj + 1) if side == "j-" else (nj, 0)
            dst = u.at[t, there, is_, inside]
            start = field.at[here - 1, :, pl.ds(k0, kq)] if first else u.at[t, here, is_, inside]
        d = 0 if side[1] == "-" else 1
        sent, received = (send_sem, recv_sem) if side[0] == "i" else (jsend_sem, jrecv_sem)
        return pltpu.make_async_remote_copy(
            src_ref=start, dst_ref=dst, send_sem=sent.at[d, t, n], recv_sem=received.at[d, t, n],
            device_id=to[side], device_id_type=MESH,
        )

    def kface(side, t, first):
        js, is_ = pl.ds(1, nj), pl.ds(1, ni)
        here, there = (TILE, TILE + nk) if side == "k-" else (nk, 0)
        start = field.at[:, :, pl.ds(here - TILE, TILE)] if first else u.at[t, js, is_, pl.ds(here, TILE)]
        d = 0 if side == "k-" else 1
        return pltpu.make_async_remote_copy(
            src_ref=start, dst_ref=u.at[t, js, is_, pl.ds(there, TILE)],
            send_sem=ksend_sem.at[d, t], recv_sem=krecv_sem.at[d, t],
            device_id=to[side], device_id_type=MESH,
        )

    def fine_of(t, n):
        low, done = sum(coarse[:n]), sum(coarse[:n + 1])
        return [m for m in range(len(parts[t])) if low <= sum(parts[t][:m]) < done]

    def send_i(t, n, first, towards=("i-", "i+")):
        for side in towards:
            @pl.when(has[side])
            def _():
                for m in fine_of(t, n):
                    face(side, t, m, first).start()

    def send_others(t, n, first):
        for side in ("j-", "j+"):
            @pl.when(has[side])
            def _():
                face(side, t, n, first).start()

        low, high = edges_of(n)

        @pl.when(low & has["k-"])
        def _():
            kface("k-", t, first).start()

        @pl.when(high & has["k+"])
        def _():
            kface("k+", t, first).start()

    def wait_i(t, n):
        for side in ("i-", "i+"):
            @pl.when(has[opposite[side]])
            def _():
                face(side, t, n, False).wait_recv()

    def wait_others(t, n):
        for side in ("j-", "j+"):
            @pl.when(has[opposite[side]])
            def _():
                face(side, t, n, False).wait_recv()

        low, high = edges_of(n)

        @pl.when(high & has["k+"])
        def _():
            kface("k-", t, False).wait_recv()

        @pl.when(low & has["k-"])
        def _():
            kface("k+", t, False).wait_recv()

    def wait_sent_i(t, who):
        for side in ("i-", "i+"):
            @pl.when(who & has[side])
            def _():
                for n in range(len(parts[t])):
                    face(side, t, n, False).wait_send()

    def wait_sent(t):
        wait_sent_i(t, first_core if t == YIELD else True)
        for side in ("j-", "j+"):
            @pl.when(has[side])
            def _():
                for n in range(len(coarse)):
                    face(side, t, n, False).wait_send()

        for side in ("k-", "k+"):
            @pl.when(has[side])
            def _():
                kface(side, t, False).wait_send()

    for n in range(len(coarse)):
        send_i(0, n, True, ("i-",))

    @pl.when(has["i+"])
    def _():
        pl.semaphore_wait(ready_sem.at[rows - 1], 1)

    for n in range(len(coarse)):
        send_i(0, n, True, ("i+",))

    @pl.when(has["k+"])
    def _():
        pl.semaphore_wait(ready_sem.at[rows], 1)

    for off in range(1, rows):
        @pl.when(row + off < rows)
        def _():
            pl.semaphore_wait(ready_sem.at[off - 1], 1)

    for n in range(len(coarse)):
        send_others(0, n, True)
    for copy in loads:
        copy.start()

    def zero_plane(t, j, i):
        u[t, j, i, pl.ds(TILE, nk)] = jnp.zeros((nk, u.shape[-1]), u.dtype)

    @pl.loop(0, STEPS)
    def _(t):
        for side, i in (("i-", 0), ("i+", ni + 1)):
            @pl.when(jnp.logical_not(has[side]))
            def _():
                @pl.loop(0, nj)
                def _(j):
                    zero_plane(t, j + 1, i)

        for side, j in (("j-", 0), ("j+", nj + 1)):
            @pl.when(jnp.logical_not(has[side]))
            def _():
                for i in range(ni):
                    zero_plane(t, j, i + 1)

        for side, k in (("k-", 0), ("k+", TILE + nk)):
            @pl.when(jnp.logical_not(has[side]))
            def _():
                @pl.loop(0, nj)
                def _(j):
                    for i in range(ni):
                        u[t, j + 1, i + 1, pl.ds(k, TILE)] = jnp.zeros((TILE, u.shape[-1]), u.dtype)

    for copy in loads:
        copy.wait()

    def stencil(t, j, i, k0, kq, skip=(False, False)):
        inner = pl.ds(pl.multiple_of(TILE + k0, TILE), kq)
        tall = u[t, j + 1, i + 1, pl.ds(k0, kq + 2 * TILE)]
        middle = tall[TILE:TILE + kq]
        spread = u[t, j, i + 1, inner] + u[t, j + 2, i + 1, inner]
        for beside, left_out in ((i, skip[0]), (i + 2, skip[1])):
            if not left_out:
                spread = spread + u[t, j + 1, beside, inner]
        spread = spread + tall[TILE - 1:TILE - 1 + kq] + tall[TILE + 1:TILE + 1 + kq]
        spread = spread - 6.0 * middle
        own_k = pl.ds(k0, kq)
        return middle + cond[j, i, own_k] * spread + src[j, i, own_k]

    def middle_step(t, n):
        k0, kq = start_of(coarse, n), coarse[n]
        for m in fine_of(t, n):
            wait_i(t, m)
        wait_others(t, n)

        @pl.loop(0, nj)
        def _(jj):
            j = lax.rem(jj + nj - 1, nj)
            for i in range(ni):
                u[t + 1, j + 1, i + 1, pl.ds(pl.multiple_of(TILE + k0, TILE), kq)] = stencil(t, j, i, k0, kq)

        if t == YIELD and n == 0:
            wait_sent_i(t, jnp.logical_not(first_core))

            @pl.when(jnp.logical_not(first_core))
            def _():
                pl.delay(PAUSE)

        send_i(t + 1, n, False)
        send_others(t + 1, n, False)

    for t in range(STEPS - 1):
        for n in range(len(coarse)):
            middle_step(t, n)
        if t > 0:
            wait_sent(t - 1)

    t = STEPS - 1
    final = parts[t]
    groups = [(inner, len(outer), coarse, n, n) for n in range(len(coarse))] if inner else []
    groups += [(outer, 0, final, n, len(coarse) + n) for n in range(len(final) - 1)]

    def stats_copy(off, group):
        planes, at, of, n, sem = group
        place = (slice(None), pl.ds(at, len(planes)), pl.ds(start_of(of, n), of[n]))
        return pltpu.make_async_remote_copy(
            src_ref=own.at[place], dst_ref=others.at[(off - 1,) + place],
            send_sem=ssend_sem.at[off - 1, sem], recv_sem=srecv_sem.at[off - 1, sem],
            device_id={"rows": lax.rem(row + off, rows)}, device_id_type=MESH,
        )

    def blocks(of, n):
        def wrap(body):
            k0 = start_of(of, n)

            @pl.loop(0, of[n] // TILE)
            def _(b):
                body(pl.multiple_of(k0 + b * TILE, TILE), pl.multiple_of(b * TILE, TILE))
        return wrap

    def sums_of(news):
        mean = sum(news[1:], news[0]) / nj
        aways = [new - mean for new in news]
        squares = [away * away for away in aways]
        return mean, sum(squares[1:], squares[0])

    def inner_step(group):
        planes, at, of, n, _ = group

        @blocks(of, n)
        def _(k, b):
            ks = pl.ds(k, TILE)
            for p, i in enumerate(planes):
                news = [stencil(t, j, i, k, TILE) for j in range(nj)]
                own[0, at + p, ks], own[1, at + p, ks] = sums_of(news)
                for j in range(nj):
                    last[j, i, ks] = news[j]

        for off in range(1, rows):
            stats_copy(off, group).start()

    def outer_ahead(n):
        @blocks(coarse, n)
        def _(k, b):
            for i in outer:
                for j in range(nj):
                    last[j, i, pl.ds(k, TILE)] = stencil(t, j, i, k, TILE, skip=(i == 0, i == ni - 1))

    def outer_step(n, into):
        @blocks(final, n)
        def _(k, b):
            ks, inside = pl.ds(k, TILE), pl.ds(pl.multiple_of(TILE + k, TILE), TILE)
            for p, i in enumerate(outer):
                faces = [face for face, here in ((0, i == 0), (ni + 1, i == ni - 1)) if here]
                news = []
                for j in range(nj):
                    arrived = [u[t, j + 1, face, inside] for face in faces]
                    news.append(last[j, i, ks] + cond[j, i, ks] * sum(arrived[1:], arrived[0]))
                if into is own:
                    own[0, p, ks], own[1, p, ks] = sums_of(news)
                else:
                    into[0, p, pl.ds(b, TILE)], into[1, p, pl.ds(b, TILE)] = sums_of(news)
                for j in range(nj):
                    last[j, i, ks] = news[j]

    def finish(group):
        planes, at, of, n, _ = group
        for off in range(1, rows):
            stats_copy(off, group).wait_recv()

        @blocks(of, n)
        def _(k, b):
            ks = pl.ds(k, TILE)
            for p, i in enumerate(planes):
                means = [own[0, at + p, ks]] + [others[off - 1, 0, at + p, ks] for off in range(1, rows)]
                spreads = [own[1, at + p, ks]] + [others[off - 1, 1, at + p, ks] for off in range(1, rows)]
                mean, scale = joined(nj, means, spreads)
                for j in range(nj):
                    scaled[j, i, ks] = (last[j, i, ks] - mean) * scale

    for n in range(len(coarse)):
        wait_others(t, n)
    count = len(coarse) if inner else 0
    for group in groups[:count]:
        inner_step(group)
    for n in range(len(coarse)):
        outer_ahead(n)
    for group in groups[:count]:
        finish(group)
    wait_sent(STEPS - 2)
    for n in range(len(final) - 1):
        wait_i(t, n)
        outer_step(n, own)
        for off in range(1, rows):
            stats_copy(off, groups[count + n]).start()
        if n > 0:
            finish(groups[count + n - 1])
    wait_i(t, len(final) - 1)
    outer_step(len(final) - 1, late)
    if len(final) > 1:
        finish(groups[-1])
    for group in groups:
        for off in range(1, rows):
            stats_copy(off, group).wait_send()
    wait_sent(t)


def planes_of(ni):
    outer = tuple(range(ni)) if ni < 3 else (0, ni - 1)
    return outer, tuple(i for i in range(ni) if i not in outer)


def joined(nj, means, spreads):
    count = len(means)
    mean = sum(means[1:], means[0]) / count
    spread = sum(spreads[1:], spreads[0])
    for other in means:
        spread = spread + nj * ((other - mean) * (other - mean))
    return mean, lax.rsqrt(spread / (nj * count) + 0.0001)


def late_start(nk, size):
    descending = lax.rem(lax.axis_index("slabs"), 2) == 0
    return pl.multiple_of(jnp.where(descending, 0, nk - size), TILE)


def write_out(late, near_anomaly, near_field, anomaly, field_end, sems):
    nj, ni, nk, _ = near_field.shape
    pieces = sems.shape[1]
    depth = nj // pieces
    outer, inner = planes_of(ni)
    places = [(0, (pl.ds(piece * depth, depth),)) for piece in range(pieces)]
    if inner:
        places += [(1, (pl.ds(piece * depth, depth), pl.ds(inner[0], len(inner)))) for piece in range(pieces)]
    if late < nk:
        early = pl.ds(pl.multiple_of(jnp.where(late_start(nk, late) == 0, late, 0), TILE), nk - late)
        places += [(1, (slice(None), i, early)) for i in outer]
    copies = []
    for at, (which, place) in enumerate(places):
        start, dst = ((near_field, field_end), (near_anomaly, anomaly))[which]
        copies.append(pltpu.make_async_copy(start.at[place], dst.at[place], sems.at[at // pieces, at % pieces]))
        copies[-1].start()
    for copy in copies:
        copy.wait()


def write_late(before, near_field, late, *refs):
    others, (anomaly, scaled, sems) = refs[:-3], refs[-3:]
    nj, ni, nk, _ = near_field.shape
    size = late.shape[2]
    start = late_start(nk, size)
    copies = []
    for b in range(size // TILE):
        ks, ms = pl.ds(b * TILE, TILE), pl.ds(pl.multiple_of(start + b * TILE, TILE), TILE)
        for p, i in enumerate(planes_of(ni)[0]):
            stats = (late,) + others
            mean, scale = joined(nj, [of[0, p, ks] for of in stats], [of[1, p, ks] for of in stats])
            for j in range(nj):
                scaled[p, j, ks] = (near_field[j, i, ms] - mean) * scale
            copies.append(pltpu.make_async_copy(scaled.at[p, :, ks], anomaly.at[:, i, ms], sems.at[p, b]))
            copies[-1].start()
    for copy in copies:
        copy.wait()


def parts_of(nk):
    half = nk // 2 if nk % (2 * TILE) == 0 else nk
    coarse = (half,) * (nk // half)
    fine, left = [], half
    for eighths in FINE:
        size = half * eighths // 8 // TILE * TILE
        if 0 < size < left:
            fine.append(size)
            left -= size
    return coarse, (coarse,) * (STEPS - 1) + (coarse[:-1] + tuple(fine) + (left,),)


def on_device(field_values, conductance, source):
    sizes = tuple(lax.axis_size(name) for name in ("rows", "cols", "slabs"))
    nj, ni, nk, levels = field_values.shape
    coarse, parts = parts_of(nk)
    most = max(len(of) for of in parts)
    groups = len(parts[-1]) + len(coarse)
    peers = max(sizes[0] - 1, 1)
    whole = pltpu.VMEM(field_values.shape, field_values.dtype)
    near = pl.BlockSpec(memory_space=pltpu.VMEM)
    outer = len(planes_of(ni)[0])
    small = (2, outer, parts[-1][-1], levels)
    anywhere = pl.BlockSpec(memory_space=pl.ANY)
    scaled, last, late = pl.pallas_call(
        functools.partial(kernel, sizes, coarse, parts),
        out_shape=(whole, whole, pltpu.VMEM(small, jnp.float32)),
        in_specs=[anywhere] * 3,
        out_specs=(near, near, near),
        scratch_shapes=[
            pltpu.VMEM((STEPS, nj + 2, ni + 2, nk + 2 * TILE, levels), jnp.float32),
            pltpu.VMEM((nj, ni, nk, levels), jnp.float32),
            pltpu.VMEM((nj, ni, nk, levels), jnp.float32),
            pltpu.VMEM((2, ni, nk, levels), jnp.float32),
            pltpu.VMEM((peers, 2, ni, nk, levels), jnp.float32),
            pltpu.SemaphoreType.DMA((3,)),
            pltpu.SemaphoreType.DMA((2, STEPS, most)),
            pltpu.SemaphoreType.DMA((2, STEPS, most)),
            pltpu.SemaphoreType.DMA((2, STEPS, len(coarse))),
            pltpu.SemaphoreType.DMA((2, STEPS, len(coarse))),
            pltpu.SemaphoreType.DMA((2, STEPS)),
            pltpu.SemaphoreType.DMA((2, STEPS)),
            pltpu.SemaphoreType.DMA((peers, groups)),
            pltpu.SemaphoreType.DMA((peers, groups)),
            pltpu.SemaphoreType.REGULAR((sizes[0] + 1,)),
        ],
        compiler_params=pltpu.CompilerParams(
            collective_id=0, has_side_effects=True, vmem_limit_bytes=52 * 1024 * 1024
        ),
        name="heat_steps",
    )(field_values, conductance, source)
    n = sizes[0]
    others = [lax.ppermute(late, "rows", [(r, (r + off) % n) for r in range(n)]) for off in range(1, n)]
    there = jax.ShapeDtypeStruct(field_values.shape, field_values.dtype)
    pieces = PIECES if nj % PIECES == 0 else 1
    size = nj * ni * nk * levels
    anomaly, field_end = pl.pallas_call(
        functools.partial(write_out, small[2]),
        out_shape=(there, there),
        in_specs=[near] * 2,
        out_specs=(anywhere, anywhere),
        scratch_shapes=[pltpu.SemaphoreType.DMA((2 + -(-outer // pieces), pieces))],
        compiler_params=pltpu.CompilerParams(vmem_limit_bytes=1024 * 1024),
        cost_estimate=pl.CostEstimate(flops=0, bytes_accessed=16 * size, transcendentals=0),
        name="write_out",
    )(scaled, last)
    anomaly = pl.pallas_call(
        write_late,
        out_shape=there,
        in_specs=[anywhere] + [near] * (2 + len(others)),
        out_specs=anywhere,
        input_output_aliases={0: 0},
        scratch_shapes=[pltpu.VMEM((outer, nj) + small[2:], jnp.float32), pltpu.SemaphoreType.DMA((outer, small[2] // TILE))],
        compiler_params=pltpu.CompilerParams(vmem_limit_bytes=2 * 1024 * 1024),
        name="write_late",
    )(anomaly, last, late, *others)
    return anomaly, field_end


def solution(mesh):
    spec = P(("trial", "rows"), "cols", "slabs", None)
    return jax.shard_map(
        on_device, mesh=mesh, in_specs=(spec,) * 3, out_specs=(spec, spec), check_vma=False
    )
```

```python
import functools

import jax
import jax.numpy as jnp
from jax import lax
from jax.experimental import pallas as pl
from jax.experimental.pallas import tpu as pltpu
from jax.sharding import PartitionSpec as P

STEPS = 4
TILE = 8
PIECES = 4
FINE = (4,)
YIELD = 1
PAUSE = 1000
MESH = pl.DeviceIdType.MESH


def kernel(
    sizes, coarse, parts, field, conductance, source, scaled, last, late,
    u, cond, src, own, others,
    load_sem, send_sem, recv_sem, jsend_sem, jrecv_sem, ksend_sem, krecv_sem, ssend_sem, srecv_sem, ready_sem,
):
    rows, cols, slabs = sizes
    nj, ni, nk, _ = field.shape
    row, col, slab = (lax.axis_index(name) for name in ("rows", "cols", "slabs"))
    has = {
        "i-": col > 0, "i+": col < cols - 1,
        "j-": row > 0, "j+": row < rows - 1,
        "k-": slab > 0, "k+": slab < slabs - 1,
    }
    to = {
        "i-": {"cols": jnp.maximum(col - 1, 0)}, "i+": {"cols": jnp.minimum(col + 1, cols - 1)},
        "j-": {"rows": jnp.maximum(row - 1, 0)}, "j+": {"rows": jnp.minimum(row + 1, rows - 1)},
        "k-": {"slabs": jnp.maximum(slab - 1, 0)}, "k+": {"slabs": jnp.minimum(slab + 1, slabs - 1)},
    }
    opposite = {"i-": "i+", "i+": "i-", "j-": "j+", "j+": "j-", "k-": "k+", "k+": "k-"}
    first_core = lax.rem(lax.axis_index("trial"), 2) == 0
    descending = lax.rem(slab, 2) == 0

    def start_of(of, n):
        before, size = sum(of[:n]), of[n]
        return pl.multiple_of(jnp.where(descending, nk - before - size, before), TILE)

    outer, inner = planes_of(ni)
    loads = [
        pltpu.make_async_copy(field, u.at[0, pl.ds(1, nj), pl.ds(1, ni), pl.ds(TILE, nk)], load_sem.at[0]),
        pltpu.make_async_copy(conductance, cond, load_sem.at[1]),
        pltpu.make_async_copy(source, src, load_sem.at[2]),
    ]

    barrier = pltpu.get_barrier_semaphore()
    for off in range(1, rows):
        @pl.when(row + off < rows)
        def _():
            pl.semaphore_signal(barrier, inc=1, device_id={"rows": jnp.minimum(row + off, rows - 1)}, device_id_type=MESH)

    expected = row
    for side in ("i", "k"):
        expected = expected + jnp.where(has[side + "-"], 1, 0)

        @pl.when(has[side + "+"])
        def _():
            pl.semaphore_signal(barrier, inc=1, device_id=to[side + "+"], device_id_type=MESH)


    @pl.when(expected > 0)
    def _():
        pl.semaphore_wait(barrier, expected)

    for side, at in (("i", rows - 1), ("k", rows)):
        @pl.when(has[side + "-"])
        def _():
            pl.semaphore_signal(ready_sem.at[at], inc=1, device_id=to[side + "-"], device_id_type=MESH)

    for off in range(1, rows):
        @pl.when(row >= off)
        def _():
            pl.semaphore_signal(
                ready_sem.at[off - 1], inc=1, device_id={"rows": jnp.maximum(row - off, 0)}, device_id_type=MESH
            )

    def edges_of(n):
        first, final = n == 0, n == len(coarse) - 1
        low = jnp.where(descending, final, first)
        high = jnp.where(descending, first, final)
        return low, high

    def face(side, t, n, first):
        of = parts[t] if side[0] == "i" else coarse
        k0, kq = start_of(of, n), of[n]
        inside = pl.ds(pl.multiple_of(TILE + k0, TILE), kq)
        js, is_ = pl.ds(1, nj), pl.ds(1, ni)
        if side[0] == "i":
            here, there = (1, ni + 1) if side == "i-" else (ni, 0)
            dst = u.at[t, js, there, inside]
            start = field.at[:, here - 1, pl.ds(k0, kq)] if first else u.at[t, js, here, inside]
        else:
            here, there = (1, nj + 1) if side == "j-" else (nj, 0)
            dst = u.at[t, there, is_, inside]
            start = field.at[here - 1, :, pl.ds(k0, kq)] if first else u.at[t, here, is_, inside]
        d = 0 if side[1] == "-" else 1
        sent, received = (send_sem, recv_sem) if side[0] == "i" else (jsend_sem, jrecv_sem)
        return pltpu.make_async_remote_copy(
            src_ref=start, dst_ref=dst, send_sem=sent.at[d, t, n], recv_sem=received.at[d, t, n],
            device_id=to[side], device_id_type=MESH,
        )

    def kface(side, t, first):
        js, is_ = pl.ds(1, nj), pl.ds(1, ni)
        here, there = (TILE, TILE + nk) if side == "k-" else (nk, 0)
        start = field.at[:, :, pl.ds(here - TILE, TILE)] if first else u.at[t, js, is_, pl.ds(here, TILE)]
        d = 0 if side == "k-" else 1
        return pltpu.make_async_remote_copy(
            src_ref=start, dst_ref=u.at[t, js, is_, pl.ds(there, TILE)],
            send_sem=ksend_sem.at[d, t], recv_sem=krecv_sem.at[d, t],
            device_id=to[side], device_id_type=MESH,
        )

    def fine_of(t, n):
        low, done = sum(coarse[:n]), sum(coarse[:n + 1])
        return [m for m in range(len(parts[t])) if low <= sum(parts[t][:m]) < done]

    def send_i(t, n, first, towards=("i-", "i+")):
        for side in towards:
            @pl.when(has[side])
            def _():
                for m in fine_of(t, n):
                    face(side, t, m, first).start()

    def send_others(t, n, first):
        for side in ("j-", "j+"):
            @pl.when(has[side])
            def _():
                face(side, t, n, first).start()

        low, high = edges_of(n)

        @pl.when(low & has["k-"])
        def _():
            kface("k-", t, first).start()

        @pl.when(high & has["k+"])
        def _():
            kface("k+", t, first).start()

    def wait_i(t, n):
        for side in ("i-", "i+"):
            @pl.when(has[opposite[side]])
            def _():
                face(side, t, n, False).wait_recv()

    def wait_others(t, n):
        for side in ("j-", "j+"):
            @pl.when(has[opposite[side]])
            def _():
                face(side, t, n, False).wait_recv()

        low, high = edges_of(n)

        @pl.when(high & has["k+"])
        def _():
            kface("k-", t, False).wait_recv()

        @pl.when(low & has["k-"])
        def _():
            kface("k+", t, False).wait_recv()

    def wait_sent_i(t, who):
        for side in ("i-", "i+"):
            @pl.when(who & has[side])
            def _():
                for n in range(len(parts[t])):
                    face(side, t, n, False).wait_send()

    def wait_sent(t):
        wait_sent_i(t, first_core if t == YIELD else True)
        for side in ("j-", "j+"):
            @pl.when(has[side])
            def _():
                for n in range(len(coarse)):
                    face(side, t, n, False).wait_send()

        for side in ("k-", "k+"):
            @pl.when(has[side])
            def _():
                kface(side, t, False).wait_send()

    for n in range(len(coarse)):
        send_i(0, n, True, ("i-",))

    @pl.when(has["i+"])
    def _():
        pl.semaphore_wait(ready_sem.at[rows - 1], 1)

    for n in range(len(coarse)):
        send_i(0, n, True, ("i+",))

    @pl.when(has["k+"])
    def _():
        pl.semaphore_wait(ready_sem.at[rows], 1)

    for off in range(1, rows):
        @pl.when(row + off < rows)
        def _():
            pl.semaphore_wait(ready_sem.at[off - 1], 1)

    for n in range(len(coarse)):
        send_others(0, n, True)
    for copy in loads:
        copy.start()

    def zero_plane(t, j, i):
        u[t, j, i, pl.ds(TILE, nk)] = jnp.zeros((nk, u.shape[-1]), u.dtype)

    @pl.loop(0, STEPS)
    def _(t):
        for side, i in (("i-", 0), ("i+", ni + 1)):
            @pl.when(jnp.logical_not(has[side]))
            def _():
                @pl.loop(0, nj)
                def _(j):
                    zero_plane(t, j + 1, i)

        for side, j in (("j-", 0), ("j+", nj + 1)):
            @pl.when(jnp.logical_not(has[side]))
            def _():
                for i in range(ni):
                    zero_plane(t, j, i + 1)

        for side, k in (("k-", 0), ("k+", TILE + nk)):
            @pl.when(jnp.logical_not(has[side]))
            def _():
                @pl.loop(0, nj)
                def _(j):
                    for i in range(ni):
                        u[t, j + 1, i + 1, pl.ds(k, TILE)] = jnp.zeros((TILE, u.shape[-1]), u.dtype)

    for copy in loads:
        copy.wait()

    def stencil(t, j, i, k0, kq, skip=(False, False)):
        inner = pl.ds(pl.multiple_of(TILE + k0, TILE), kq)
        tall = u[t, j + 1, i + 1, pl.ds(k0, kq + 2 * TILE)]
        middle = tall[TILE:TILE + kq]
        spread = u[t, j, i + 1, inner] + u[t, j + 2, i + 1, inner]
        for beside, left_out in ((i, skip[0]), (i + 2, skip[1])):
            if not left_out:
                spread = spread + u[t, j + 1, beside, inner]
        spread = spread + tall[TILE - 1:TILE - 1 + kq] + tall[TILE + 1:TILE + 1 + kq]
        spread = spread - 6.0 * middle
        own_k = pl.ds(k0, kq)
        return middle + cond[j, i, own_k] * spread + src[j, i, own_k]

    def middle_step(t, n):
        k0, kq = start_of(coarse, n), coarse[n]
        for m in fine_of(t, n):
            wait_i(t, m)
        wait_others(t, n)

        @pl.loop(0, nj)
        def _(jj):
            j = lax.rem(jj + nj - 1, nj)
            for i in range(ni):
                u[t + 1, j + 1, i + 1, pl.ds(pl.multiple_of(TILE + k0, TILE), kq)] = stencil(t, j, i, k0, kq)

        if t == YIELD and n == 0:
            wait_sent_i(t, jnp.logical_not(first_core))

            @pl.when(jnp.logical_not(first_core))
            def _():
                pl.delay(PAUSE)

        send_i(t + 1, n, False)
        send_others(t + 1, n, False)

    for t in range(STEPS - 1):
        for n in range(len(coarse)):
            middle_step(t, n)
        if t > 0:
            wait_sent(t - 1)

    t = STEPS - 1
    final = parts[t]
    groups = [(inner, len(outer), coarse, n, n) for n in range(len(coarse))] if inner else []
    groups += [(outer, 0, final, n, len(coarse) + n) for n in range(len(final) - 1)]

    def stats_copy(off, group):
        planes, at, of, n, sem = group
        place = (slice(None), pl.ds(at, len(planes)), pl.ds(start_of(of, n), of[n]))
        return pltpu.make_async_remote_copy(
            src_ref=own.at[place], dst_ref=others.at[(off - 1,) + place],
            send_sem=ssend_sem.at[off - 1, sem], recv_sem=srecv_sem.at[off - 1, sem],
            device_id={"rows": lax.rem(row + off, rows)}, device_id_type=MESH,
        )

    def blocks(of, n):
        def wrap(body):
            k0 = start_of(of, n)

            @pl.loop(0, of[n] // TILE)
            def _(b):
                body(pl.multiple_of(k0 + b * TILE, TILE), pl.multiple_of(b * TILE, TILE))
        return wrap

    def sums_of(news):
        mean = sum(news[1:], news[0]) / nj
        aways = [new - mean for new in news]
        squares = [away * away for away in aways]
        return mean, sum(squares[1:], squares[0])

    def inner_step(group):
        planes, at, of, n, _ = group

        @blocks(of, n)
        def _(k, b):
            ks = pl.ds(k, TILE)
            for p, i in enumerate(planes):
                news = [stencil(t, j, i, k, TILE) for j in range(nj)]
                own[0, at + p, ks], own[1, at + p, ks] = sums_of(news)
                for j in range(nj):
                    last[j, i, ks] = news[j]

        for off in range(1, rows):
            stats_copy(off, group).start()

    def outer_ahead(n):
        @blocks(coarse, n)
        def _(k, b):
            for i in outer:
                for j in range(nj):
                    last[j, i, pl.ds(k, TILE)] = stencil(t, j, i, k, TILE, skip=(i == 0, i == ni - 1))

    def outer_step(n, into):
        @blocks(final, n)
        def _(k, b):
            ks, inside = pl.ds(k, TILE), pl.ds(pl.multiple_of(TILE + k, TILE), TILE)
            for p, i in enumerate(outer):
                faces = [face for face, here in ((0, i == 0), (ni + 1, i == ni - 1)) if here]
                news = []
                for j in range(nj):
                    arrived = [u[t, j + 1, face, inside] for face in faces]
                    news.append(last[j, i, ks] + cond[j, i, ks] * sum(arrived[1:], arrived[0]))
                if into is own:
                    own[0, p, ks], own[1, p, ks] = sums_of(news)
                else:
                    into[0, p, pl.ds(b, TILE)], into[1, p, pl.ds(b, TILE)] = sums_of(news)
                for j in range(nj):
                    last[j, i, ks] = news[j]

    def finish(group):
        planes, at, of, n, _ = group
        for off in range(1, rows):
            stats_copy(off, group).wait_recv()

        @blocks(of, n)
        def _(k, b):
            ks = pl.ds(k, TILE)
            for p, i in enumerate(planes):
                means = [own[0, at + p, ks]] + [others[off - 1, 0, at + p, ks] for off in range(1, rows)]
                spreads = [own[1, at + p, ks]] + [others[off - 1, 1, at + p, ks] for off in range(1, rows)]
                mean, scale = joined(nj, means, spreads)
                for j in range(nj):
                    scaled[j, i, ks] = (last[j, i, ks] - mean) * scale

    for n in range(len(coarse)):
        wait_others(t, n)
    count = len(coarse) if inner else 0
    for group in groups[:count]:
        inner_step(group)
    for n in range(len(coarse)):
        outer_ahead(n)
    for group in groups[:count]:
        finish(group)
    wait_sent(STEPS - 2)
    for n in range(len(final) - 1):
        wait_i(t, n)
        outer_step(n, own)
        for off in range(1, rows):
            stats_copy(off, groups[count + n]).start()
        if n > 0:
            finish(groups[count + n - 1])
    first_rows = row < rows // 2
    if len(final) > 1:
        @pl.when(jnp.logical_not(first_rows))
        def _():
            finish(groups[-1])

    wait_i(t, len(final) - 1)
    outer_step(len(final) - 1, late)
    if len(final) > 1:
        @pl.when(first_rows)
        def _():
            finish(groups[-1])

    for group in groups:
        for off in range(1, rows):
            stats_copy(off, group).wait_send()
    wait_sent(t)


def planes_of(ni):
    outer = tuple(range(ni)) if ni < 3 else (0, ni - 1)
    return outer, tuple(i for i in range(ni) if i not in outer)


def joined(nj, means, spreads):
    count = len(means)
    mean = sum(means[1:], means[0]) / count
    spread = sum(spreads[1:], spreads[0])
    for other in means:
        spread = spread + nj * ((other - mean) * (other - mean))
    return mean, lax.rsqrt(spread / (nj * count) + 0.0001)


def late_start(nk, size):
    descending = lax.rem(lax.axis_index("slabs"), 2) == 0
    return pl.multiple_of(jnp.where(descending, 0, nk - size), TILE)


def write_out(late, near_anomaly, near_field, anomaly, field_end, sems):
    nj, ni, nk, _ = near_field.shape
    pieces = sems.shape[1]
    depth = nj // pieces
    outer, inner = planes_of(ni)
    places = [(0, (pl.ds(piece * depth, depth),)) for piece in range(pieces)]
    if inner:
        places += [(1, (pl.ds(piece * depth, depth), pl.ds(inner[0], len(inner)))) for piece in range(pieces)]
    if late < nk:
        early = pl.ds(pl.multiple_of(jnp.where(late_start(nk, late) == 0, late, 0), TILE), nk - late)
        places += [(1, (slice(None), i, early)) for i in outer]
    copies = []
    for at, (which, place) in enumerate(places):
        start, dst = ((near_field, field_end), (near_anomaly, anomaly))[which]
        copies.append(pltpu.make_async_copy(start.at[place], dst.at[place], sems.at[at // pieces, at % pieces]))
        copies[-1].start()
    for copy in copies:
        copy.wait()


def write_late(before, near_field, late, *refs):
    others, (anomaly, scaled, sems) = refs[:-3], refs[-3:]
    nj, ni, nk, _ = near_field.shape
    size = late.shape[2]
    start = late_start(nk, size)
    copies = []
    for b in range(size // TILE):
        ks, ms = pl.ds(b * TILE, TILE), pl.ds(pl.multiple_of(start + b * TILE, TILE), TILE)
        for p, i in enumerate(planes_of(ni)[0]):
            stats = (late,) + others
            mean, scale = joined(nj, [of[0, p, ks] for of in stats], [of[1, p, ks] for of in stats])
            for j in range(nj):
                scaled[p, j, ks] = (near_field[j, i, ms] - mean) * scale
            copies.append(pltpu.make_async_copy(scaled.at[p, :, ks], anomaly.at[:, i, ms], sems.at[p, b]))
            copies[-1].start()
    for copy in copies:
        copy.wait()


def parts_of(nk):
    half = nk // 2 if nk % (2 * TILE) == 0 else nk
    coarse = (half,) * (nk // half)
    fine, left = [], half
    for eighths in FINE:
        size = half * eighths // 8 // TILE * TILE
        if 0 < size < left:
            fine.append(size)
            left -= size
    return coarse, (coarse,) * (STEPS - 1) + (coarse[:-1] + tuple(fine) + (left,),)


def on_device(field_values, conductance, source):
    sizes = tuple(lax.axis_size(name) for name in ("rows", "cols", "slabs"))
    nj, ni, nk, levels = field_values.shape
    coarse, parts = parts_of(nk)
    most = max(len(of) for of in parts)
    groups = len(parts[-1]) + len(coarse)
    peers = max(sizes[0] - 1, 1)
    whole = pltpu.VMEM(field_values.shape, field_values.dtype)
    near = pl.BlockSpec(memory_space=pltpu.VMEM)
    outer = len(planes_of(ni)[0])
    small = (2, outer, parts[-1][-1], levels)
    anywhere = pl.BlockSpec(memory_space=pl.ANY)
    scaled, last, late = pl.pallas_call(
        functools.partial(kernel, sizes, coarse, parts),
        out_shape=(whole, whole, pltpu.VMEM(small, jnp.float32)),
        in_specs=[anywhere] * 3,
        out_specs=(near, near, near),
        scratch_shapes=[
            pltpu.VMEM((STEPS, nj + 2, ni + 2, nk + 2 * TILE, levels), jnp.float32),
            pltpu.VMEM((nj, ni, nk, levels), jnp.float32),
            pltpu.VMEM((nj, ni, nk, levels), jnp.float32),
            pltpu.VMEM((2, ni, nk, levels), jnp.float32),
            pltpu.VMEM((peers, 2, ni, nk, levels), jnp.float32),
            pltpu.SemaphoreType.DMA((3,)),
            pltpu.SemaphoreType.DMA((2, STEPS, most)),
            pltpu.SemaphoreType.DMA((2, STEPS, most)),
            pltpu.SemaphoreType.DMA((2, STEPS, len(coarse))),
            pltpu.SemaphoreType.DMA((2, STEPS, len(coarse))),
            pltpu.SemaphoreType.DMA((2, STEPS)),
            pltpu.SemaphoreType.DMA((2, STEPS)),
            pltpu.SemaphoreType.DMA((peers, groups)),
            pltpu.SemaphoreType.DMA((peers, groups)),
            pltpu.SemaphoreType.REGULAR((sizes[0] + 1,)),
        ],
        compiler_params=pltpu.CompilerParams(
            collective_id=0, has_side_effects=True, vmem_limit_bytes=52 * 1024 * 1024
        ),
        name="heat_steps",
    )(field_values, conductance, source)
    n = sizes[0]
    others = [lax.ppermute(late, "rows", [(r, (r + off) % n) for r in range(n)]) for off in range(1, n)]
    there = jax.ShapeDtypeStruct(field_values.shape, field_values.dtype)
    pieces = PIECES if nj % PIECES == 0 else 1
    size = nj * ni * nk * levels
    anomaly, field_end = pl.pallas_call(
        functools.partial(write_out, small[2]),
        out_shape=(there, there),
        in_specs=[near] * 2,
        out_specs=(anywhere, anywhere),
        scratch_shapes=[pltpu.SemaphoreType.DMA((2 + -(-outer // pieces), pieces))],
        compiler_params=pltpu.CompilerParams(vmem_limit_bytes=1024 * 1024),
        cost_estimate=pl.CostEstimate(flops=0, bytes_accessed=16 * size, transcendentals=0),
        name="write_out",
    )(scaled, last)
    anomaly = pl.pallas_call(
        write_late,
        out_shape=there,
        in_specs=[anywhere] + [near] * (2 + len(others)),
        out_specs=anywhere,
        input_output_aliases={0: 0},
        scratch_shapes=[pltpu.VMEM((outer, nj) + small[2:], jnp.float32), pltpu.SemaphoreType.DMA((outer, small[2] // TILE))],
        compiler_params=pltpu.CompilerParams(vmem_limit_bytes=2 * 1024 * 1024),
        name="write_late",
    )(anomaly, last, late, *others)
    return anomaly, field_end


def solution(mesh):
    spec = P(("trial", "rows"), "cols", "slabs", None)
    return jax.shard_map(
        on_device, mesh=mesh, in_specs=(spec,) * 3, out_specs=(spec, spec), check_vma=False
    )
```

```python
import functools

import jax
import jax.numpy as jnp
from jax import lax
from jax.experimental import pallas as pl
from jax.experimental.pallas import tpu as pltpu
from jax.sharding import PartitionSpec as P

STEPS = 4
TILE = 8
PIECES = 4
FINE = (4, 3)
LATE = 2
YIELD = 1
PAUSE = 1300
MESH = pl.DeviceIdType.MESH


def kernel(
    sizes, coarse, parts, field, conductance, source, scaled, last, late,
    u, cond, src, own, others,
    load_sem, send_sem, recv_sem, jsend_sem, jrecv_sem, ksend_sem, krecv_sem, ssend_sem, srecv_sem, ready_sem,
):
    rows, cols, slabs = sizes
    nj, ni, nk, _ = field.shape
    row, col, slab = (lax.axis_index(name) for name in ("rows", "cols", "slabs"))
    has = {
        "i-": col > 0, "i+": col < cols - 1,
        "j-": row > 0, "j+": row < rows - 1,
        "k-": slab > 0, "k+": slab < slabs - 1,
    }
    to = {
        "i-": {"cols": jnp.maximum(col - 1, 0)}, "i+": {"cols": jnp.minimum(col + 1, cols - 1)},
        "j-": {"rows": jnp.maximum(row - 1, 0)}, "j+": {"rows": jnp.minimum(row + 1, rows - 1)},
        "k-": {"slabs": jnp.maximum(slab - 1, 0)}, "k+": {"slabs": jnp.minimum(slab + 1, slabs - 1)},
    }
    opposite = {"i-": "i+", "i+": "i-", "j-": "j+", "j+": "j-", "k-": "k+", "k+": "k-"}
    first_core = lax.rem(lax.axis_index("trial"), 2) == 0
    descending = lax.rem(slab, 2) == 0

    def start_of(of, n):
        before, size = sum(of[:n]), of[n]
        return pl.multiple_of(jnp.where(descending, nk - before - size, before), TILE)

    outer, inner = planes_of(ni)
    loads = [
        pltpu.make_async_copy(field, u.at[0, pl.ds(1, nj), pl.ds(1, ni), pl.ds(TILE, nk)], load_sem.at[0]),
        pltpu.make_async_copy(conductance, cond, load_sem.at[1]),
        pltpu.make_async_copy(source, src, load_sem.at[2]),
    ]

    barrier = pltpu.get_barrier_semaphore()
    for off in range(1, rows):
        @pl.when(row + off < rows)
        def _():
            pl.semaphore_signal(barrier, inc=1, device_id={"rows": jnp.minimum(row + off, rows - 1)}, device_id_type=MESH)

    expected = row
    for side in ("i", "k"):
        expected = expected + jnp.where(has[side + "-"], 1, 0)

        @pl.when(has[side + "+"])
        def _():
            pl.semaphore_signal(barrier, inc=1, device_id=to[side + "+"], device_id_type=MESH)


    @pl.when(expected > 0)
    def _():
        pl.semaphore_wait(barrier, expected)

    for side, at in (("i", rows - 1), ("k", rows)):
        @pl.when(has[side + "-"])
        def _():
            pl.semaphore_signal(ready_sem.at[at], inc=1, device_id=to[side + "-"], device_id_type=MESH)

    for off in range(1, rows):
        @pl.when(row >= off)
        def _():
            pl.semaphore_signal(
                ready_sem.at[off - 1], inc=1, device_id={"rows": jnp.maximum(row - off, 0)}, device_id_type=MESH
            )

    def edges_of(n):
        first, final = n == 0, n == len(coarse) - 1
        low = jnp.where(descending, final, first)
        high = jnp.where(descending, first, final)
        return low, high

    def face(side, t, n, first):
        of = parts[t] if side[0] == "i" else coarse
        k0, kq = start_of(of, n), of[n]
        inside = pl.ds(pl.multiple_of(TILE + k0, TILE), kq)
        js, is_ = pl.ds(1, nj), pl.ds(1, ni)
        if side[0] == "i":
            here, there = (1, ni + 1) if side == "i-" else (ni, 0)
            dst = u.at[t, js, there, inside]
            start = field.at[:, here - 1, pl.ds(k0, kq)] if first else u.at[t, js, here, inside]
        else:
            here, there = (1, nj + 1) if side == "j-" else (nj, 0)
            dst = u.at[t, there, is_, inside]
            start = field.at[here - 1, :, pl.ds(k0, kq)] if first else u.at[t, here, is_, inside]
        d = 0 if side[1] == "-" else 1
        sent, received = (send_sem, recv_sem) if side[0] == "i" else (jsend_sem, jrecv_sem)
        return pltpu.make_async_remote_copy(
            src_ref=start, dst_ref=dst, send_sem=sent.at[d, t, n], recv_sem=received.at[d, t, n],
            device_id=to[side], device_id_type=MESH,
        )

    def kface(side, t, first):
        js, is_ = pl.ds(1, nj), pl.ds(1, ni)
        here, there = (TILE, TILE + nk) if side == "k-" else (nk, 0)
        start = field.at[:, :, pl.ds(here - TILE, TILE)] if first else u.at[t, js, is_, pl.ds(here, TILE)]
        d = 0 if side == "k-" else 1
        return pltpu.make_async_remote_copy(
            src_ref=start, dst_ref=u.at[t, js, is_, pl.ds(there, TILE)],
            send_sem=ksend_sem.at[d, t], recv_sem=krecv_sem.at[d, t],
            device_id=to[side], device_id_type=MESH,
        )

    def fine_of(t, n):
        low, done = sum(coarse[:n]), sum(coarse[:n + 1])
        return [m for m in range(len(parts[t])) if low <= sum(parts[t][:m]) < done]

    def send_i(t, n, first, towards=("i-", "i+")):
        for side in towards:
            @pl.when(has[side])
            def _():
                for m in fine_of(t, n):
                    face(side, t, m, first).start()

    def send_others(t, n, first):
        for side in ("j-", "j+"):
            @pl.when(has[side])
            def _():
                face(side, t, n, first).start()

        low, high = edges_of(n)

        @pl.when(low & has["k-"])
        def _():
            kface("k-", t, first).start()

        @pl.when(high & has["k+"])
        def _():
            kface("k+", t, first).start()

    def wait_i(t, n):
        for side in ("i-", "i+"):
            @pl.when(has[opposite[side]])
            def _():
                face(side, t, n, False).wait_recv()

    def wait_others(t, n):
        for side in ("j-", "j+"):
            @pl.when(has[opposite[side]])
            def _():
                face(side, t, n, False).wait_recv()

        low, high = edges_of(n)

        @pl.when(high & has["k+"])
        def _():
            kface("k-", t, False).wait_recv()

        @pl.when(low & has["k-"])
        def _():
            kface("k+", t, False).wait_recv()

    def wait_sent_i(t, who):
        for side in ("i-", "i+"):
            @pl.when(who & has[side])
            def _():
                for n in range(len(parts[t])):
                    face(side, t, n, False).wait_send()

    def wait_sent(t):
        wait_sent_i(t, first_core if t == YIELD else True)
        for side in ("j-", "j+"):
            @pl.when(has[side])
            def _():
                for n in range(len(coarse)):
                    face(side, t, n, False).wait_send()

        for side in ("k-", "k+"):
            @pl.when(has[side])
            def _():
                kface(side, t, False).wait_send()

    for n in range(len(coarse)):
        send_i(0, n, True, ("i-",))

    @pl.when(has["i+"])
    def _():
        pl.semaphore_wait(ready_sem.at[rows - 1], 1)

    for n in range(len(coarse)):
        send_i(0, n, True, ("i+",))

    @pl.when(has["k+"])
    def _():
        pl.semaphore_wait(ready_sem.at[rows], 1)

    for off in range(1, rows):
        @pl.when(row + off < rows)
        def _():
            pl.semaphore_wait(ready_sem.at[off - 1], 1)

    for n in range(len(coarse)):
        send_others(0, n, True)
    for copy in loads:
        copy.start()

    def zero_plane(t, j, i):
        u[t, j, i, pl.ds(TILE, nk)] = jnp.zeros((nk, u.shape[-1]), u.dtype)

    @pl.loop(0, STEPS)
    def _(t):
        for side, i in (("i-", 0), ("i+", ni + 1)):
            @pl.when(jnp.logical_not(has[side]))
            def _():
                @pl.loop(0, nj)
                def _(j):
                    zero_plane(t, j + 1, i)

        for side, j in (("j-", 0), ("j+", nj + 1)):
            @pl.when(jnp.logical_not(has[side]))
            def _():
                for i in range(ni):
                    zero_plane(t, j, i + 1)

        for side, k in (("k-", 0), ("k+", TILE + nk)):
            @pl.when(jnp.logical_not(has[side]))
            def _():
                @pl.loop(0, nj)
                def _(j):
                    for i in range(ni):
                        u[t, j + 1, i + 1, pl.ds(k, TILE)] = jnp.zeros((TILE, u.shape[-1]), u.dtype)

    for copy in loads:
        copy.wait()

    def stencil(t, j, i, k0, kq, skip=(False, False)):
        inner = pl.ds(pl.multiple_of(TILE + k0, TILE), kq)
        tall = u[t, j + 1, i + 1, pl.ds(k0, kq + 2 * TILE)]
        middle = tall[TILE:TILE + kq]
        spread = u[t, j, i + 1, inner] + u[t, j + 2, i + 1, inner]
        for beside, left_out in ((i, skip[0]), (i + 2, skip[1])):
            if not left_out:
                spread = spread + u[t, j + 1, beside, inner]
        spread = spread + tall[TILE - 1:TILE - 1 + kq] + tall[TILE + 1:TILE + 1 + kq]
        spread = spread - 6.0 * middle
        own_k = pl.ds(k0, kq)
        return middle + cond[j, i, own_k] * spread + src[j, i, own_k]

    def middle_step(t, n):
        k0, kq = start_of(coarse, n), coarse[n]
        for m in fine_of(t, n):
            wait_i(t, m)
        wait_others(t, n)

        @pl.loop(0, nj)
        def _(jj):
            j = lax.rem(jj + nj - 1, nj)
            for i in range(ni):
                u[t + 1, j + 1, i + 1, pl.ds(pl.multiple_of(TILE + k0, TILE), kq)] = stencil(t, j, i, k0, kq)

        if t == YIELD and n == 0:
            wait_sent_i(t, jnp.logical_not(first_core))

            @pl.when(jnp.logical_not(first_core))
            def _():
                pl.delay(PAUSE)

        send_i(t + 1, n, False)
        send_others(t + 1, n, False)

    for t in range(STEPS - 1):
        for n in range(len(coarse)):
            middle_step(t, n)
        if t > 0:
            wait_sent(t - 1)

    t = STEPS - 1
    final = parts[t]
    prompt = len(final) - min(LATE, len(final))
    groups = [(inner, len(outer), coarse, n, n) for n in range(len(coarse))] if inner else []
    groups += [(outer, 0, final, n, len(coarse) + n) for n in range(prompt)]

    def stats_copy(off, group):
        planes, at, of, n, sem = group
        place = (slice(None), pl.ds(at, len(planes)), pl.ds(start_of(of, n), of[n]))
        return pltpu.make_async_remote_copy(
            src_ref=own.at[place], dst_ref=others.at[(off - 1,) + place],
            send_sem=ssend_sem.at[off - 1, sem], recv_sem=srecv_sem.at[off - 1, sem],
            device_id={"rows": lax.rem(row + off, rows)}, device_id_type=MESH,
        )

    def blocks(of, n):
        def wrap(body):
            k0 = start_of(of, n)

            @pl.loop(0, of[n] // TILE)
            def _(b):
                body(pl.multiple_of(k0 + b * TILE, TILE), pl.multiple_of(b * TILE, TILE))
        return wrap

    def sums_of(news):
        mean = sum(news[1:], news[0]) / nj
        aways = [new - mean for new in news]
        squares = [away * away for away in aways]
        return mean, sum(squares[1:], squares[0])

    def inner_step(group):
        planes, at, of, n, _ = group

        @blocks(of, n)
        def _(k, b):
            ks = pl.ds(k, TILE)
            for p, i in enumerate(planes):
                news = [stencil(t, j, i, k, TILE) for j in range(nj)]
                own[0, at + p, ks], own[1, at + p, ks] = sums_of(news)
                for j in range(nj):
                    last[j, i, ks] = news[j]

        for off in range(1, rows):
            stats_copy(off, group).start()

    def outer_ahead(n):
        @blocks(coarse, n)
        def _(k, b):
            for i in outer:
                for j in range(nj):
                    last[j, i, pl.ds(k, TILE)] = stencil(t, j, i, k, TILE, skip=(i == 0, i == ni - 1))

    def outer_step(n):
        @blocks(final, n)
        def _(k, b):
            ks, inside = pl.ds(k, TILE), pl.ds(pl.multiple_of(TILE + k, TILE), TILE)
            for p, i in enumerate(outer):
                faces = [face for face, here in ((0, i == 0), (ni + 1, i == ni - 1)) if here]
                news = []
                for j in range(nj):
                    arrived = [u[t, j + 1, face, inside] for face in faces]
                    news.append(last[j, i, ks] + cond[j, i, ks] * sum(arrived[1:], arrived[0]))
                if n < prompt:
                    own[0, p, ks], own[1, p, ks] = sums_of(news)
                else:
                    at = pl.ds(pl.multiple_of(k - late_start(nk, late.shape[2]), TILE), TILE)
                    late[0, p, at], late[1, p, at] = sums_of(news)
                for j in range(nj):
                    last[j, i, ks] = news[j]

    def finish(group):
        planes, at, of, n, _ = group
        for off in range(1, rows):
            stats_copy(off, group).wait_recv()

        @blocks(of, n)
        def _(k, b):
            ks = pl.ds(k, TILE)
            for p, i in enumerate(planes):
                means = [own[0, at + p, ks]] + [others[off - 1, 0, at + p, ks] for off in range(1, rows)]
                spreads = [own[1, at + p, ks]] + [others[off - 1, 1, at + p, ks] for off in range(1, rows)]
                mean, scale = joined(nj, means, spreads)
                for j in range(nj):
                    scaled[j, i, ks] = (last[j, i, ks] - mean) * scale

    for n in range(len(coarse)):
        wait_others(t, n)
    count = len(coarse) if inner else 0
    for group in groups[:count]:
        inner_step(group)
    for n in range(len(coarse)):
        outer_ahead(n)
    for group in groups[:count]:
        finish(group)
    wait_sent(STEPS - 2)
    for n in range(prompt):
        wait_i(t, n)
        outer_step(n)
        for off in range(1, rows):
            stats_copy(off, groups[count + n]).start()
        if n > 0:
            finish(groups[count + n - 1])
    first_rows = row < rows // 2
    if prompt > 0:
        @pl.when(jnp.logical_not(first_rows))
        def _():
            finish(groups[-1])

    for n in range(prompt, len(final)):
        wait_i(t, n)
        outer_step(n)
    if prompt > 0:
        @pl.when(first_rows)
        def _():
            finish(groups[-1])

    for group in groups:
        for off in range(1, rows):
            stats_copy(off, group).wait_send()
    wait_sent(t)


def planes_of(ni):
    outer = tuple(range(ni)) if ni < 3 else (0, ni - 1)
    return outer, tuple(i for i in range(ni) if i not in outer)


def joined(nj, means, spreads):
    count = len(means)
    mean = sum(means[1:], means[0]) / count
    spread = sum(spreads[1:], spreads[0])
    for other in means:
        spread = spread + nj * ((other - mean) * (other - mean))
    return mean, lax.rsqrt(spread / (nj * count) + 0.0001)


def late_start(nk, size):
    descending = lax.rem(lax.axis_index("slabs"), 2) == 0
    return pl.multiple_of(jnp.where(descending, 0, nk - size), TILE)


def write_out(late, near_anomaly, near_field, anomaly, field_end, sems):
    nj, ni, nk, _ = near_field.shape
    pieces = sems.shape[1]
    depth = nj // pieces
    outer, inner = planes_of(ni)
    places = [(0, (pl.ds(piece * depth, depth),)) for piece in range(pieces)]
    if inner:
        places += [(1, (pl.ds(piece * depth, depth), pl.ds(inner[0], len(inner)))) for piece in range(pieces)]
    if late < nk:
        early = pl.ds(pl.multiple_of(jnp.where(late_start(nk, late) == 0, late, 0), TILE), nk - late)
        places += [(1, (slice(None), i, early)) for i in outer]
    copies = []
    for at, (which, place) in enumerate(places):
        start, dst = ((near_field, field_end), (near_anomaly, anomaly))[which]
        copies.append(pltpu.make_async_copy(start.at[place], dst.at[place], sems.at[at // pieces, at % pieces]))
        copies[-1].start()
    for copy in copies:
        copy.wait()


def write_late(before, near_field, late, *refs):
    others, (anomaly, scaled, sems) = refs[:-3], refs[-3:]
    nj, ni, nk, _ = near_field.shape
    size = late.shape[2]
    start = late_start(nk, size)
    copies = []
    for b in range(size // TILE):
        ks, ms = pl.ds(b * TILE, TILE), pl.ds(pl.multiple_of(start + b * TILE, TILE), TILE)
        for p, i in enumerate(planes_of(ni)[0]):
            stats = (late,) + others
            mean, scale = joined(nj, [of[0, p, ks] for of in stats], [of[1, p, ks] for of in stats])
            for j in range(nj):
                scaled[p, j, ks] = (near_field[j, i, ms] - mean) * scale
            copies.append(pltpu.make_async_copy(scaled.at[p, :, ks], anomaly.at[:, i, ms], sems.at[p, b]))
            copies[-1].start()
    for copy in copies:
        copy.wait()


def parts_of(nk):
    half = nk // 2 if nk % (2 * TILE) == 0 else nk
    coarse = (half,) * (nk // half)
    fine, left = [], half
    for eighths in FINE:
        size = half * eighths // 8 // TILE * TILE
        if 0 < size < left:
            fine.append(size)
            left -= size
    return coarse, (coarse,) * (STEPS - 1) + (coarse[:-1] + tuple(fine) + (left,),)


def on_device(field_values, conductance, source):
    sizes = tuple(lax.axis_size(name) for name in ("rows", "cols", "slabs"))
    nj, ni, nk, levels = field_values.shape
    coarse, parts = parts_of(nk)
    most = max(len(of) for of in parts)
    groups = len(parts[-1]) + len(coarse)
    peers = max(sizes[0] - 1, 1)
    whole = pltpu.VMEM(field_values.shape, field_values.dtype)
    near = pl.BlockSpec(memory_space=pltpu.VMEM)
    outer = len(planes_of(ni)[0])
    small = (2, outer, sum(parts[-1][-LATE:]), levels)
    anywhere = pl.BlockSpec(memory_space=pl.ANY)
    scaled, last, late = pl.pallas_call(
        functools.partial(kernel, sizes, coarse, parts),
        out_shape=(whole, whole, pltpu.VMEM(small, jnp.float32)),
        in_specs=[anywhere] * 3,
        out_specs=(near, near, near),
        scratch_shapes=[
            pltpu.VMEM((STEPS, nj + 2, ni + 2, nk + 2 * TILE, levels), jnp.float32),
            pltpu.VMEM((nj, ni, nk, levels), jnp.float32),
            pltpu.VMEM((nj, ni, nk, levels), jnp.float32),
            pltpu.VMEM((2, ni, nk, levels), jnp.float32),
            pltpu.VMEM((peers, 2, ni, nk, levels), jnp.float32),
            pltpu.SemaphoreType.DMA((3,)),
            pltpu.SemaphoreType.DMA((2, STEPS, most)),
            pltpu.SemaphoreType.DMA((2, STEPS, most)),
            pltpu.SemaphoreType.DMA((2, STEPS, len(coarse))),
            pltpu.SemaphoreType.DMA((2, STEPS, len(coarse))),
            pltpu.SemaphoreType.DMA((2, STEPS)),
            pltpu.SemaphoreType.DMA((2, STEPS)),
            pltpu.SemaphoreType.DMA((peers, groups)),
            pltpu.SemaphoreType.DMA((peers, groups)),
            pltpu.SemaphoreType.REGULAR((sizes[0] + 1,)),
        ],
        compiler_params=pltpu.CompilerParams(
            collective_id=0, has_side_effects=True, vmem_limit_bytes=52 * 1024 * 1024
        ),
        name="heat_steps",
    )(field_values, conductance, source)
    n = sizes[0]
    others = [lax.ppermute(late, "rows", [(r, (r + off) % n) for r in range(n)]) for off in range(1, n)]
    there = jax.ShapeDtypeStruct(field_values.shape, field_values.dtype)
    pieces = PIECES if nj % PIECES == 0 else 1
    size = nj * ni * nk * levels
    anomaly, field_end = pl.pallas_call(
        functools.partial(write_out, small[2]),
        out_shape=(there, there),
        in_specs=[near] * 2,
        out_specs=(anywhere, anywhere),
        scratch_shapes=[pltpu.SemaphoreType.DMA((2 + -(-outer // pieces), pieces))],
        compiler_params=pltpu.CompilerParams(vmem_limit_bytes=1024 * 1024),
        cost_estimate=pl.CostEstimate(flops=0, bytes_accessed=16 * size, transcendentals=0),
        name="write_out",
    )(scaled, last)
    anomaly = pl.pallas_call(
        write_late,
        out_shape=there,
        in_specs=[anywhere] + [near] * (2 + len(others)),
        out_specs=anywhere,
        input_output_aliases={0: 0},
        scratch_shapes=[pltpu.VMEM((outer, nj) + small[2:], jnp.float32), pltpu.SemaphoreType.DMA((outer, small[2] // TILE))],
        compiler_params=pltpu.CompilerParams(vmem_limit_bytes=2 * 1024 * 1024),
        name="write_late",
    )(anomaly, last, late, *others)
    return anomaly, field_end


def solution(mesh):
    spec = P(("trial", "rows"), "cols", "slabs", None)
    return jax.shard_map(
        on_device, mesh=mesh, in_specs=(spec,) * 3, out_specs=(spec, spec), check_vma=False
    )
```

```python
import functools

import jax
import jax.numpy as jnp
from jax import lax
from jax.experimental import pallas as pl
from jax.experimental.pallas import tpu as pltpu
from jax.sharding import PartitionSpec as P

STEPS = 4
TILE = 8
PIECES = 2
FINE = (4, 3)
LATE = 2
YIELD = 1
PAUSE = 1300
MESH = pl.DeviceIdType.MESH


def kernel(
    sizes, coarse, parts, field, conductance, source, scaled, last, late,
    u, cond, src, own, others,
    load_sem, send_sem, recv_sem, jsend_sem, jrecv_sem, ksend_sem, krecv_sem, ssend_sem, srecv_sem, ready_sem,
):
    rows, cols, slabs = sizes
    nj, ni, nk, _ = field.shape
    row, col, slab = (lax.axis_index(name) for name in ("rows", "cols", "slabs"))
    has = {
        "i-": col > 0, "i+": col < cols - 1,
        "j-": row > 0, "j+": row < rows - 1,
        "k-": slab > 0, "k+": slab < slabs - 1,
    }
    to = {
        "i-": {"cols": jnp.maximum(col - 1, 0)}, "i+": {"cols": jnp.minimum(col + 1, cols - 1)},
        "j-": {"rows": jnp.maximum(row - 1, 0)}, "j+": {"rows": jnp.minimum(row + 1, rows - 1)},
        "k-": {"slabs": jnp.maximum(slab - 1, 0)}, "k+": {"slabs": jnp.minimum(slab + 1, slabs - 1)},
    }
    opposite = {"i-": "i+", "i+": "i-", "j-": "j+", "j+": "j-", "k-": "k+", "k+": "k-"}
    first_core = lax.rem(lax.axis_index("trial"), 2) == 0
    descending = lax.rem(slab, 2) == 0

    def start_of(of, n):
        before, size = sum(of[:n]), of[n]
        return pl.multiple_of(jnp.where(descending, nk - before - size, before), TILE)

    outer, inner = planes_of(ni)
    loads = [
        pltpu.make_async_copy(field, u.at[0, pl.ds(1, nj), pl.ds(1, ni), pl.ds(TILE, nk)], load_sem.at[0]),
        pltpu.make_async_copy(conductance, cond, load_sem.at[1]),
        pltpu.make_async_copy(source, src, load_sem.at[2]),
    ]

    barrier = pltpu.get_barrier_semaphore()
    for off in range(1, rows):
        @pl.when(row + off < rows)
        def _():
            pl.semaphore_signal(barrier, inc=1, device_id={"rows": jnp.minimum(row + off, rows - 1)}, device_id_type=MESH)

    expected = row
    for side in ("i", "k"):
        expected = expected + jnp.where(has[side + "-"], 1, 0)

        @pl.when(has[side + "+"])
        def _():
            pl.semaphore_signal(barrier, inc=1, device_id=to[side + "+"], device_id_type=MESH)


    @pl.when(expected > 0)
    def _():
        pl.semaphore_wait(barrier, expected)

    for side, at in (("i", rows - 1), ("k", rows)):
        @pl.when(has[side + "-"])
        def _():
            pl.semaphore_signal(ready_sem.at[at], inc=1, device_id=to[side + "-"], device_id_type=MESH)

    for off in range(1, rows):
        @pl.when(row >= off)
        def _():
            pl.semaphore_signal(
                ready_sem.at[off - 1], inc=1, device_id={"rows": jnp.maximum(row - off, 0)}, device_id_type=MESH
            )

    def edges_of(n):
        first, final = n == 0, n == len(coarse) - 1
        low = jnp.where(descending, final, first)
        high = jnp.where(descending, first, final)
        return low, high

    def face(side, t, n, first):
        of = parts[t] if side[0] == "i" else coarse
        k0, kq = start_of(of, n), of[n]
        inside = pl.ds(pl.multiple_of(TILE + k0, TILE), kq)
        js, is_ = pl.ds(1, nj), pl.ds(1, ni)
        if side[0] == "i":
            here, there = (1, ni + 1) if side == "i-" else (ni, 0)
            dst = u.at[t, js, there, inside]
            start = field.at[:, here - 1, pl.ds(k0, kq)] if first else u.at[t, js, here, inside]
        else:
            here, there = (1, nj + 1) if side == "j-" else (nj, 0)
            dst = u.at[t, there, is_, inside]
            start = field.at[here - 1, :, pl.ds(k0, kq)] if first else u.at[t, here, is_, inside]
        d = 0 if side[1] == "-" else 1
        sent, received = (send_sem, recv_sem) if side[0] == "i" else (jsend_sem, jrecv_sem)
        return pltpu.make_async_remote_copy(
            src_ref=start, dst_ref=dst, send_sem=sent.at[d, t, n], recv_sem=received.at[d, t, n],
            device_id=to[side], device_id_type=MESH,
        )

    def kface(side, t, first):
        js, is_ = pl.ds(1, nj), pl.ds(1, ni)
        here, there = (TILE, TILE + nk) if side == "k-" else (nk, 0)
        start = field.at[:, :, pl.ds(here - TILE, TILE)] if first else u.at[t, js, is_, pl.ds(here, TILE)]
        d = 0 if side == "k-" else 1
        return pltpu.make_async_remote_copy(
            src_ref=start, dst_ref=u.at[t, js, is_, pl.ds(there, TILE)],
            send_sem=ksend_sem.at[d, t], recv_sem=krecv_sem.at[d, t],
            device_id=to[side], device_id_type=MESH,
        )

    def fine_of(t, n):
        low, done = sum(coarse[:n]), sum(coarse[:n + 1])
        return [m for m in range(len(parts[t])) if low <= sum(parts[t][:m]) < done]

    def send_i(t, n, first, towards=("i-", "i+")):
        for side in towards:
            @pl.when(has[side])
            def _():
                for m in fine_of(t, n):
                    face(side, t, m, first).start()

    def send_others(t, n, first):
        for side in ("j-", "j+"):
            @pl.when(has[side])
            def _():
                face(side, t, n, first).start()

        low, high = edges_of(n)

        @pl.when(low & has["k-"])
        def _():
            kface("k-", t, first).start()

        @pl.when(high & has["k+"])
        def _():
            kface("k+", t, first).start()

    def wait_i(t, n):
        for side in ("i-", "i+"):
            @pl.when(has[opposite[side]])
            def _():
                face(side, t, n, False).wait_recv()

    def wait_others(t, n):
        for side in ("j-", "j+"):
            @pl.when(has[opposite[side]])
            def _():
                face(side, t, n, False).wait_recv()

        low, high = edges_of(n)

        @pl.when(high & has["k+"])
        def _():
            kface("k-", t, False).wait_recv()

        @pl.when(low & has["k-"])
        def _():
            kface("k+", t, False).wait_recv()

    def wait_sent_i(t, who):
        for side in ("i-", "i+"):
            @pl.when(who & has[side])
            def _():
                for n in range(len(parts[t])):
                    face(side, t, n, False).wait_send()

    def wait_sent(t):
        wait_sent_i(t, first_core if t == YIELD else True)
        for side in ("j-", "j+"):
            @pl.when(has[side])
            def _():
                for n in range(len(coarse)):
                    face(side, t, n, False).wait_send()

        for side in ("k-", "k+"):
            @pl.when(has[side])
            def _():
                kface(side, t, False).wait_send()

    for n in range(len(coarse)):
        send_i(0, n, True, ("i-",))

    @pl.when(has["i+"])
    def _():
        pl.semaphore_wait(ready_sem.at[rows - 1], 1)

    for n in range(len(coarse)):
        send_i(0, n, True, ("i+",))

    @pl.when(has["k+"])
    def _():
        pl.semaphore_wait(ready_sem.at[rows], 1)

    for off in range(1, rows):
        @pl.when(row + off < rows)
        def _():
            pl.semaphore_wait(ready_sem.at[off - 1], 1)

    for n in range(len(coarse)):
        send_others(0, n, True)
    for copy in loads:
        copy.start()

    def zero_plane(t, j, i):
        u[t, j, i, pl.ds(TILE, nk)] = jnp.zeros((nk, u.shape[-1]), u.dtype)

    @pl.loop(0, STEPS)
    def _(t):
        for side, i in (("i-", 0), ("i+", ni + 1)):
            @pl.when(jnp.logical_not(has[side]))
            def _():
                @pl.loop(0, nj)
                def _(j):
                    zero_plane(t, j + 1, i)

        for side, j in (("j-", 0), ("j+", nj + 1)):
            @pl.when(jnp.logical_not(has[side]))
            def _():
                for i in range(ni):
                    zero_plane(t, j, i + 1)

        for side, k in (("k-", 0), ("k+", TILE + nk)):
            @pl.when(jnp.logical_not(has[side]))
            def _():
                @pl.loop(0, nj)
                def _(j):
                    for i in range(ni):
                        u[t, j + 1, i + 1, pl.ds(k, TILE)] = jnp.zeros((TILE, u.shape[-1]), u.dtype)

    for copy in loads:
        copy.wait()

    def stencil(t, j, i, k0, kq, skip=(False, False)):
        inner = pl.ds(pl.multiple_of(TILE + k0, TILE), kq)
        tall = u[t, j + 1, i + 1, pl.ds(k0, kq + 2 * TILE)]
        middle = tall[TILE:TILE + kq]
        spread = u[t, j, i + 1, inner] + u[t, j + 2, i + 1, inner]
        for beside, left_out in ((i, skip[0]), (i + 2, skip[1])):
            if not left_out:
                spread = spread + u[t, j + 1, beside, inner]
        spread = spread + tall[TILE - 1:TILE - 1 + kq] + tall[TILE + 1:TILE + 1 + kq]
        spread = spread - 6.0 * middle
        own_k = pl.ds(k0, kq)
        return middle + cond[j, i, own_k] * spread + src[j, i, own_k]

    def middle_step(t, n):
        k0, kq = start_of(coarse, n), coarse[n]
        for m in fine_of(t, n):
            wait_i(t, m)
        wait_others(t, n)

        @pl.loop(0, nj)
        def _(jj):
            j = lax.rem(jj + nj - 1, nj)
            for i in range(ni):
                u[t + 1, j + 1, i + 1, pl.ds(pl.multiple_of(TILE + k0, TILE), kq)] = stencil(t, j, i, k0, kq)

        if t == YIELD and n == 0:
            wait_sent_i(t, jnp.logical_not(first_core))

            @pl.when(jnp.logical_not(first_core))
            def _():
                pl.delay(PAUSE)

        send_i(t + 1, n, False)
        send_others(t + 1, n, False)

    for t in range(STEPS - 1):
        for n in range(len(coarse)):
            middle_step(t, n)
        if t > 0:
            wait_sent(t - 1)

    t = STEPS - 1
    final = parts[t]
    prompt = len(final) - min(LATE, len(final))
    groups = [(inner, len(outer), coarse, n, n) for n in range(len(coarse))] if inner else []
    groups += [(outer, 0, final, n, len(coarse) + n) for n in range(prompt)]

    def stats_copy(off, group):
        planes, at, of, n, sem = group
        place = (slice(None), pl.ds(at, len(planes)), pl.ds(start_of(of, n), of[n]))
        return pltpu.make_async_remote_copy(
            src_ref=own.at[place], dst_ref=others.at[(off - 1,) + place],
            send_sem=ssend_sem.at[off - 1, sem], recv_sem=srecv_sem.at[off - 1, sem],
            device_id={"rows": lax.rem(row + off, rows)}, device_id_type=MESH,
        )

    def blocks(of, n):
        def wrap(body):
            k0 = start_of(of, n)

            @pl.loop(0, of[n] // TILE)
            def _(b):
                body(pl.multiple_of(k0 + b * TILE, TILE), pl.multiple_of(b * TILE, TILE))
        return wrap

    def sums_of(news):
        mean = sum(news[1:], news[0]) / nj
        aways = [new - mean for new in news]
        squares = [away * away for away in aways]
        return mean, sum(squares[1:], squares[0])

    def inner_step(group):
        planes, at, of, n, _ = group

        @blocks(of, n)
        def _(k, b):
            ks = pl.ds(k, TILE)
            for p, i in enumerate(planes):
                news = [stencil(t, j, i, k, TILE) for j in range(nj)]
                own[0, at + p, ks], own[1, at + p, ks] = sums_of(news)
                for j in range(nj):
                    last[j, i, ks] = news[j]

        for off in range(1, rows):
            stats_copy(off, group).start()

    def outer_ahead(n):
        @blocks(coarse, n)
        def _(k, b):
            for i in outer:
                for j in range(nj):
                    last[j, i, pl.ds(k, TILE)] = stencil(t, j, i, k, TILE, skip=(i == 0, i == ni - 1))

    def outer_step(n):
        @blocks(final, n)
        def _(k, b):
            ks, inside = pl.ds(k, TILE), pl.ds(pl.multiple_of(TILE + k, TILE), TILE)
            for p, i in enumerate(outer):
                faces = [face for face, here in ((0, i == 0), (ni + 1, i == ni - 1)) if here]
                news = []
                for j in range(nj):
                    arrived = [u[t, j + 1, face, inside] for face in faces]
                    news.append(last[j, i, ks] + cond[j, i, ks] * sum(arrived[1:], arrived[0]))
                if n < prompt:
                    own[0, p, ks], own[1, p, ks] = sums_of(news)
                else:
                    at = pl.ds(pl.multiple_of(k - late_start(nk, late.shape[2]), TILE), TILE)
                    late[0, p, at], late[1, p, at] = sums_of(news)
                for j in range(nj):
                    last[j, i, ks] = news[j]

    def finish(group):
        planes, at, of, n, _ = group
        for off in range(1, rows):
            stats_copy(off, group).wait_recv()

        @blocks(of, n)
        def _(k, b):
            ks = pl.ds(k, TILE)
            for p, i in enumerate(planes):
                means = [own[0, at + p, ks]] + [others[off - 1, 0, at + p, ks] for off in range(1, rows)]
                spreads = [own[1, at + p, ks]] + [others[off - 1, 1, at + p, ks] for off in range(1, rows)]
                mean, scale = joined(nj, means, spreads)
                for j in range(nj):
                    scaled[j, i, ks] = (last[j, i, ks] - mean) * scale

    for n in range(len(coarse)):
        wait_others(t, n)
    count = len(coarse) if inner else 0
    for group in groups[:count]:
        inner_step(group)
    for n in range(len(coarse)):
        outer_ahead(n)
    for group in groups[:count]:
        finish(group)
    wait_sent(STEPS - 2)
    for n in range(prompt):
        wait_i(t, n)
        outer_step(n)
        for off in range(1, rows):
            stats_copy(off, groups[count + n]).start()
        if n > 0:
            finish(groups[count + n - 1])
    first_rows = row < rows // 2
    if prompt > 0:
        @pl.when(jnp.logical_not(first_rows))
        def _():
            finish(groups[-1])

    for n in range(prompt, len(final)):
        wait_i(t, n)
        outer_step(n)
    if prompt > 0:
        @pl.when(first_rows)
        def _():
            finish(groups[-1])

    for group in groups:
        for off in range(1, rows):
            stats_copy(off, group).wait_send()
    wait_sent(t)


def planes_of(ni):
    outer = tuple(range(ni)) if ni < 3 else (0, ni - 1)
    return outer, tuple(i for i in range(ni) if i not in outer)


def joined(nj, means, spreads):
    count = len(means)
    mean = sum(means[1:], means[0]) / count
    spread = sum(spreads[1:], spreads[0])
    for other in means:
        spread = spread + nj * ((other - mean) * (other - mean))
    return mean, lax.rsqrt(spread / (nj * count) + 0.0001)


def late_start(nk, size):
    descending = lax.rem(lax.axis_index("slabs"), 2) == 0
    return pl.multiple_of(jnp.where(descending, 0, nk - size), TILE)


def write_out(late, near_anomaly, near_field, anomaly, field_end, sems):
    nj, ni, nk, _ = near_field.shape
    pieces = sems.shape[1]
    depth = nj // pieces
    outer, inner = planes_of(ni)
    places = [(0, (pl.ds(piece * depth, depth),)) for piece in range(pieces)]
    if inner:
        places += [(1, (pl.ds(piece * depth, depth), pl.ds(inner[0], len(inner)))) for piece in range(pieces)]
    if late < nk:
        early = pl.ds(pl.multiple_of(jnp.where(late_start(nk, late) == 0, late, 0), TILE), nk - late)
        places += [(1, (slice(None), i, early)) for i in outer]
    copies = []
    for at, (which, place) in enumerate(places):
        start, dst = ((near_field, field_end), (near_anomaly, anomaly))[which]
        copies.append(pltpu.make_async_copy(start.at[place], dst.at[place], sems.at[at // pieces, at % pieces]))
        copies[-1].start()
    for copy in copies:
        copy.wait()


def write_late(before, near_field, late, *refs):
    others, (anomaly, scaled, sems) = refs[:-3], refs[-3:]
    nj, ni, nk, _ = near_field.shape
    size = late.shape[2]
    start = late_start(nk, size)
    copies = []
    for b in range(size // TILE):
        ks, ms = pl.ds(b * TILE, TILE), pl.ds(pl.multiple_of(start + b * TILE, TILE), TILE)
        for p, i in enumerate(planes_of(ni)[0]):
            stats = (late,) + others
            mean, scale = joined(nj, [of[0, p, ks] for of in stats], [of[1, p, ks] for of in stats])
            for j in range(nj):
                scaled[p, j, ks] = (near_field[j, i, ms] - mean) * scale
            copies.append(pltpu.make_async_copy(scaled.at[p, :, ks], anomaly.at[:, i, ms], sems.at[p, b]))
            copies[-1].start()
    for copy in copies:
        copy.wait()


def parts_of(nk):
    half = nk // 2 if nk % (2 * TILE) == 0 else nk
    coarse = (half,) * (nk // half)
    fine, left = [], half
    for eighths in FINE:
        size = half * eighths // 8 // TILE * TILE
        if 0 < size < left:
            fine.append(size)
            left -= size
    return coarse, (coarse,) * (STEPS - 1) + (coarse[:-1] + tuple(fine) + (left,),)


def on_device(field_values, conductance, source):
    sizes = tuple(lax.axis_size(name) for name in ("rows", "cols", "slabs"))
    nj, ni, nk, levels = field_values.shape
    coarse, parts = parts_of(nk)
    most = max(len(of) for of in parts)
    groups = len(parts[-1]) + len(coarse)
    peers = max(sizes[0] - 1, 1)
    whole = pltpu.VMEM(field_values.shape, field_values.dtype)
    near = pl.BlockSpec(memory_space=pltpu.VMEM)
    outer = len(planes_of(ni)[0])
    small = (2, outer, sum(parts[-1][-LATE:]), levels)
    anywhere = pl.BlockSpec(memory_space=pl.ANY)
    scaled, last, late = pl.pallas_call(
        functools.partial(kernel, sizes, coarse, parts),
        out_shape=(whole, whole, pltpu.VMEM(small, jnp.float32)),
        in_specs=[anywhere] * 3,
        out_specs=(near, near, near),
        scratch_shapes=[
            pltpu.VMEM((STEPS, nj + 2, ni + 2, nk + 2 * TILE, levels), jnp.float32),
            pltpu.VMEM((nj, ni, nk, levels), jnp.float32),
            pltpu.VMEM((nj, ni, nk, levels), jnp.float32),
            pltpu.VMEM((2, ni, nk, levels), jnp.float32),
            pltpu.VMEM((peers, 2, ni, nk, levels), jnp.float32),
            pltpu.SemaphoreType.DMA((3,)),
            pltpu.SemaphoreType.DMA((2, STEPS, most)),
            pltpu.SemaphoreType.DMA((2, STEPS, most)),
            pltpu.SemaphoreType.DMA((2, STEPS, len(coarse))),
            pltpu.SemaphoreType.DMA((2, STEPS, len(coarse))),
            pltpu.SemaphoreType.DMA((2, STEPS)),
            pltpu.SemaphoreType.DMA((2, STEPS)),
            pltpu.SemaphoreType.DMA((peers, groups)),
            pltpu.SemaphoreType.DMA((peers, groups)),
            pltpu.SemaphoreType.REGULAR((sizes[0] + 1,)),
        ],
        compiler_params=pltpu.CompilerParams(
            collective_id=0, has_side_effects=True, vmem_limit_bytes=52 * 1024 * 1024
        ),
        name="heat_steps",
    )(field_values, conductance, source)
    n = sizes[0]
    others = [lax.ppermute(late, "rows", [(r, (r + off) % n) for r in range(n)]) for off in range(1, n)]
    there = jax.ShapeDtypeStruct(field_values.shape, field_values.dtype)
    pieces = PIECES if nj % PIECES == 0 else 1
    size = nj * ni * nk * levels
    anomaly, field_end = pl.pallas_call(
        functools.partial(write_out, small[2]),
        out_shape=(there, there),
        in_specs=[near] * 2,
        out_specs=(anywhere, anywhere),
        scratch_shapes=[pltpu.SemaphoreType.DMA((2 + -(-outer // pieces), pieces))],
        compiler_params=pltpu.CompilerParams(vmem_limit_bytes=1024 * 1024),
        cost_estimate=pl.CostEstimate(flops=0, bytes_accessed=16 * size, transcendentals=0),
        name="write_out",
    )(scaled, last)
    anomaly = pl.pallas_call(
        write_late,
        out_shape=there,
        in_specs=[anywhere] + [near] * (2 + len(others)),
        out_specs=anywhere,
        input_output_aliases={0: 0},
        scratch_shapes=[pltpu.VMEM((outer, nj) + small[2:], jnp.float32), pltpu.SemaphoreType.DMA((outer, small[2] // TILE))],
        compiler_params=pltpu.CompilerParams(vmem_limit_bytes=2 * 1024 * 1024),
        name="write_late",
    )(anomaly, last, late, *others)
    return anomaly, field_end


def solution(mesh):
    spec = P(("trial", "rows"), "cols", "slabs", None)
    return jax.shard_map(
        on_device, mesh=mesh, in_specs=(spec,) * 3, out_specs=(spec, spec), check_vma=False
    )
```
